256 devices in a mesh: seq: 16 (over z, x_lo), img: 8 (over y, x_hi), fsdp: 2 (over core).
Axes of the slice: x: 4 (x_hi: 2, x_lo: 2; x = x_hi * 2 + x_lo), y: 4, z: 8, core: 2. Of those that a mesh axis runs over, the one named last changes fastest.
Arguments:
- vision_feats: bfloat16 [8, 2304, 1024], P('img', ('seq', 'fsdp')), may hold values from -6 to 6
- ln_gain: float32 [1024], replicated, may hold values from 0.5 to 1.5
- ln_bias: float32 [1024], replicated, may hold values from -3 to 3
- w_in: bfloat16 [1024, 4096], P('fsdp', 'seq'), may hold values from -0.1875 to 0.1875
- b_in: float32 [4096], P('seq'), may hold values from -3 to 3
- w_out: bfloat16 [4096, 4096], P('seq', 'fsdp'), may hold values from -0.09375 to 0.09375
- lm_grad: bfloat16 [8, 4096, 4096], P('img', 'seq', 'fsdp'), may hold values from -0.079589844 to 0.079589844
- image_counts: int32 [8, 2], P('img'), may hold values from 1 to 3, as said below
- token_pos: int32 [8, 2304], P('img'), may hold values from 0 to 2047, as said below
Outputs:
- w_in_grad: float32 [1024, 4096], P(('img', 'fsdp'), 'seq')
- b_in_grad: float32 [4096], replicated
- w_out_grad: float32 [4096, 4096], P(('seq', 'img'), 'fsdp')
- b_out_grad: float32 [4096], replicated
- ln_gain_grad: float32 [1024], replicated
- ln_bias_grad: float32 [1024], replicated
The draws below stay inside these ranges and needn't reach their ends.
Inputs may be any that keep to these rules, and one draw needn't show every extreme that they name: `image_counts`: in each group the 2 samples hold 4 images together, each sample one or more. `token_pos`: each image's 576 tokens take consecutive positions of its sample's sequence in order; a sample's images come in order without intersection, and images are numbered sample by sample as image_counts gives.
All inputs are finite; a program needn't handle non-finite values.
Results may differ from the reference program's by a relative error of at most 0.0047.
Values may be sent and summed in bfloat16 or wider, within the bound.
No kernel may reach another device: no remote copies, remote signals or barrier semaphores. Data moves between devices by JAX's collectives and lax.ppermute only.
A program may use at most 128 MiB of HBM per device.

```python
import jax
import jax.numpy as jnp
from jax import lax

D = 4096
DV = 1024
HID = 4096
PATCH = 576
IMGS = 4
LEN = 2048
IMG_ROWS = 2304
POS = 4096
GROUPS = 8


def image_layout(key):
    base_key = jax.random.fold_in(key, 311)
    count_key, place_key = jax.random.split(base_key)
    first_count = 1 + jax.random.randint(count_key, (GROUPS,), 0, 3)
    counts = jnp.stack([first_count, IMGS - first_count], axis=1).astype(jnp.int32)
    text_room = LEN - counts * PATCH
    marks = jax.random.randint(place_key, (GROUPS, 2, 3), 0, 1 + text_room[:, :, None])
    marks = jnp.sort(marks, axis=2).astype(jnp.int32)
    pieces = []
    for image_index in range(IMGS):
        in_second = image_index >= first_count
        sample = in_second.astype(jnp.int32)
        slot_index = jnp.where(in_second, image_index - first_count, image_index).astype(jnp.int32)
        mark_row = jnp.take_along_axis(marks, sample[:, None, None], axis=1)[:, 0, :]
        begin_pos = jnp.take_along_axis(mark_row, slot_index[:, None], axis=1)[:, 0] + slot_index * PATCH
        pieces.append(begin_pos[:, None] + jnp.arange(PATCH, dtype=jnp.int32)[None, :])
    positions = jnp.concatenate(pieces, axis=1).astype(jnp.int32)
    return (counts, positions)


def draw_image_counts(key, part):
    counts, positions = image_layout(key)
    return counts


def draw_token_pos(key, part):
    counts, positions = image_layout(key)
    return positions


def shard_levels(key, shape, cuts, low, top_value):
    def one(position, parts):
        draws = jax.random.uniform(jax.random.fold_in(jax.random.fold_in(key, 6), position), (parts,), jnp.float32, low / len(cuts), top_value / len(cuts))
        return jnp.repeat(jnp.exp(draws), shape[position] // parts).reshape((-1,) + (1,) * (len(shape) - position - 1))

    loudness = one(*cuts[0])
    for cut in cuts[1:]:
        loudness = loudness * one(*cut)
    return loudness


def normal_values(stream_key, extent, deviation, limit, cuts=(), held_as=jnp.bfloat16):
    entries = jax.random.normal(stream_key, extent, jnp.float32) * deviation
    if len(cuts) > 0:
        entries = shard_levels(stream_key, extent, cuts, -0.22, 0.18) * entries
    return jnp.clip(entries, min=-limit, max=limit).astype(held_as)


def setup_inputs(seed: int = 0) -> dict:
    arg_keys = jax.random.split(jax.random.key(seed), 10)
    return {
        "vision_feats": normal_values(arg_keys[0], (GROUPS, IMG_ROWS, DV), 1.0, 6.0, ((0, 8), (1, 32))),
        "ln_gain": jnp.clip(1.0 + 0.1 * jax.random.normal(arg_keys[1], (DV,), jnp.float32), 0.5, 1.5),
        "ln_bias": normal_values(arg_keys[2], (DV,), 0.5, 3.0, (), jnp.float32),
        "w_in": normal_values(arg_keys[3], (DV, HID), DV ** -0.5, 0.1875, ((0, 2), (1, 16))),
        "b_in": normal_values(arg_keys[4], (HID,), 0.5, 3.0, ((0, 16),), jnp.float32),
        "w_out": normal_values(arg_keys[5], (HID, D), HID ** -0.5, 0.09375, ((0, 16), (1, 2))),
        "lm_grad": normal_values(arg_keys[6], (GROUPS, POS, D), 0.01, 0.079589844, ((0, 8), (1, 16), (2, 2))),
        "image_counts": draw_image_counts(jax.random.fold_in(arg_keys[9], 71), 0),
        "token_pos": draw_token_pos(jax.random.fold_in(arg_keys[9], 71), 0),
    }


def gelu_parts(preact):
    cumul = 0.5 * (1.0 + lax.erf(preact * 0.7071067811865476))
    density = jnp.exp(-0.5 * preact * preact) * 0.3989422804014327
    return (preact * cumul, cumul + preact * density)

def layer_norm(features, ln_gain, ln_bias):
    values = features.astype(jnp.float32)
    row_mean = lax.optimization_barrier(jnp.mean(values, axis=1, keepdims=True))
    centred = values - row_mean
    row_var = lax.optimization_barrier(jnp.mean(centred * centred, axis=1, keepdims=True))
    normed = centred * lax.rsqrt(row_var + 1e-05)
    return (normed, (normed * ln_gain + ln_bias).astype(jnp.bfloat16))

def absolute_positions(counts, positions):
    row_count = positions.shape[0]
    image_index = jnp.arange(row_count, dtype=jnp.int32) // PATCH
    bounds = jnp.cumsum(counts).astype(jnp.int32)
    sample = lax.optimization_barrier(jnp.sum((image_index[:, None] >= bounds[None, :]).astype(jnp.int32), axis=1))
    return (sample * LEN + positions).astype(jnp.int32)

def contract(left, right, left_dim, right_dim):
    return lax.dot_general(left, right, (((left_dim,), (right_dim,)), ((), ())), preferred_element_type=jnp.float32)

def reference(vision_feats, ln_gain, ln_bias, w_in, b_in, w_out, lm_grad, image_counts, token_pos):

    def one_group(totals, inputs):
        features, cotangent, counts, positions = inputs
        normed, normed_in = layer_norm(features, ln_gain, ln_bias)
        preact = jnp.dot(normed_in, w_in, preferred_element_type=jnp.float32) + b_in
        activ, slope = gelu_parts(preact)
        hidden = activ.astype(jnp.bfloat16)
        picked = cotangent[absolute_positions(counts, positions)]
        hidden_grad = contract(picked, w_out, 1, 1)
        preact_grad = (hidden_grad * slope).astype(jnp.bfloat16)
        normed_grad = contract(preact_grad, w_in, 1, 1)
        terms = (contract(normed_in, preact_grad, 0, 0), lax.optimization_barrier(jnp.sum(preact_grad, axis=0, dtype=jnp.float32)), contract(hidden, picked, 0, 0), lax.optimization_barrier(jnp.sum(picked, axis=0, dtype=jnp.float32)), lax.optimization_barrier(jnp.sum(normed_grad * normed, axis=0)), lax.optimization_barrier(jnp.sum(normed_grad, axis=0)))
        return (tuple((left + right for left, right in zip(totals, terms))), None)
    start_state = (jnp.zeros((DV, HID), jnp.float32), jnp.zeros((HID,), jnp.float32), jnp.zeros((HID, D), jnp.float32), jnp.zeros((D,), jnp.float32), jnp.zeros((DV,), jnp.float32), jnp.zeros((DV,), jnp.float32))
    totals, unused = lax.scan(one_group, start_state, (vision_feats, lm_grad, image_counts, token_pos))
    return (totals[0], totals[1], totals[2], totals[3], totals[4], totals[5])
```

```python
import jax
import jax.numpy as jnp
from jax import lax
from jax.sharding import Mesh
from jax.sharding import PartitionSpec as P

PATCH = 576
LEN = 2048
SEQ = ("z", "xl")
IMG = ("y", "xh")
PLANE = ("xl", "y", "xh")


def gelu_parts(preact):
    cumul = 0.5 * (1.0 + lax.erf(preact * 0.7071067811865476))
    density = jnp.exp(-0.5 * preact * preact) * 0.3989422804014327
    return (preact * cumul, cumul + preact * density)


def contract(left, right, left_dim, right_dim):
    return lax.dot_general(
        left, right, (((left_dim,), (right_dim,)), ((), ())), preferred_element_type=jnp.float32
    )


def swap(array, axis):
    return lax.ppermute(array, axis, [(0, 1), (1, 0)])


def in_axis_order(own, other, axis):
    first = lax.axis_index(axis) == 0
    return jnp.where(first, own, other), jnp.where(first, other, own)


def ring(block, far_up):
    count = lax.axis_size("z")
    up = [(i, (i + 1) % count) for i in range(count)]
    down = [(i, (i - 1) % count) for i in range(count)]
    half = count // 2
    below, above = block, block
    held = {0: block}
    for step in range(1, half + 1):
        if step < half or far_up:
            below = lax.ppermute(below, "z", up)
            held[count - step] = below
        if step < half or not far_up:
            above = lax.ppermute(above, "z", down)
            held[step] = above
    return [held[i] for i in range(count)]


def split_terms(vector):
    high = vector.astype(jnp.bfloat16)
    low = (vector - high.astype(jnp.float32)).astype(jnp.bfloat16)
    return high, low


def per_device(vision_feats, ln_gain, ln_bias, w_in, b_in, w_out, lm_grad, image_counts, token_pos):
    z_count = lax.axis_size("z")
    z = lax.axis_index("z")
    xl = lax.axis_index("xl")
    core = lax.axis_index("c")
    vision = vision_feats[0]
    lm = lm_grad[0]
    rows, half_width = lm.shape
    feats = vision.shape[1]
    quarter = half_width // 2
    counts = image_counts[0]
    positions = token_pos[0]
    tokens = positions.shape[0]
    image_index = jnp.arange(tokens, dtype=jnp.int32) // PATCH
    abs_pos = jnp.where(image_index >= counts[0], LEN, 0) + positions
    seen = jnp.stack(ring(vision, True))
    seen = jnp.stack([seen, swap(seen, "xl")])
    seen = jnp.stack([seen, swap(seen, "c")])
    own_rows = vision.shape[0]
    terms = split_terms(b_in)
    third = (b_in - terms[0].astype(jnp.float32) - terms[1].astype(jnp.float32)).astype(jnp.bfloat16)
    w_first, w_second = in_axis_order(w_in, swap(w_in, "c"), "c")
    packed = jnp.concatenate(
        [w_first, w_second, jnp.stack([*terms, third]), jnp.zeros((5, b_in.shape[0]), jnp.bfloat16)]
    )
    packed = jnp.concatenate(in_axis_order(packed, swap(packed, "xl"), "xl"), axis=1)
    w_in_all = packed[:feats]
    b_in_all = jnp.sum(packed[feats : feats + 3].astype(jnp.float32), axis=0)
    w_out_all = jnp.concatenate(in_axis_order(w_out, swap(w_out, "xl"), "xl"), axis=0)
    hidden_width = w_out_all.shape[0]
    chunks = [ring(lm[:, :quarter], True), ring(lm[:, quarter:], False)]
    block_of = lax.rem(z + jnp.arange(z_count, dtype=jnp.int32), z_count)
    held_pos = ((2 * block_of + xl) * rows)[:, None] + jnp.arange(rows, dtype=jnp.int32)[None, :]
    held_pos = held_pos.reshape(-1)
    by_owner = abs_pos.reshape(z_count, 2, 2, own_rows)
    by_owner = jnp.concatenate([by_owner, by_owner])
    by_owner = lax.dynamic_slice_in_dim(by_owner, z, z_count, 0)
    by_owner = by_owner.transpose(2, 1, 0, 3)
    by_owner = jnp.where(xl == 0, by_owner, by_owner[:, ::-1])
    by_owner = jnp.where(core == 0, by_owner, by_owner[::-1]).reshape(-1)
    select = (held_pos[:, None] == by_owner[None, :]).astype(jnp.bfloat16)
    starts = abs_pos[::PATCH]
    inside = (held_pos[:, None] >= starts[None, :]) & (held_pos[:, None] < starts[None, :] + PATCH)
    mask = jnp.any(inside, axis=1).astype(jnp.float32)[:, None]
    placed = jnp.dot(select, seen.reshape(tokens, feats), preferred_element_type=jnp.float32)
    row_mean = jnp.mean(placed, axis=1, keepdims=True)
    centred = placed - row_mean
    row_var = jnp.mean(centred * centred, axis=1, keepdims=True)
    normed = centred * lax.rsqrt(row_var + 1e-05)
    normed_in = (normed * ln_gain + ln_bias).astype(jnp.bfloat16)
    normed = normed.astype(jnp.bfloat16)
    preact = jnp.dot(normed_in, w_in_all, preferred_element_type=jnp.float32) + b_in_all
    activ, slope = gelu_parts(preact)
    hidden = (activ * mask).astype(jnp.bfloat16)
    slope = slope * mask
    plane_count = lax.axis_size(PLANE)
    img_count = lax.axis_size(IMG)
    piece = feats // (img_count * 2)
    own = jnp.arange(feats // 2, dtype=jnp.int32)
    own = (own // piece) * (2 * piece) + core * piece + lax.rem(own, piece)
    pick = (jnp.arange(feats, dtype=jnp.int32)[:, None] == own[None, :]).astype(jnp.bfloat16)
    both = jnp.concatenate(
        [
            jnp.dot(normed_in, pick, preferred_element_type=jnp.float32).astype(jnp.bfloat16),
            jnp.dot(normed, pick, preferred_element_type=jnp.float32).astype(jnp.bfloat16),
        ],
        axis=1,
    )
    own_w_in = contract(pick, w_in_all, 0, 0)
    w_chunks = (w_out_all[:, :quarter], w_out_all[:, quarter:])
    hidden_part = jnp.concatenate(
        [
            contract(chunks[0][i], w_chunks[0], 1, 1) + contract(chunks[1][i], w_chunks[1], 1, 1)
            for i in range(z_count)
        ]
    )
    hidden_grad = hidden_part + swap(hidden_part.astype(jnp.bfloat16), "c").astype(jnp.float32)
    preact_grad = (hidden_grad * slope).astype(jnp.bfloat16)
    w_out_parts = []
    for chunk in chunks:
        total = 0.0
        for i in range(z_count):
            total = total + contract(hidden[i * rows : (i + 1) * rows], chunk[i], 0, 0)
        w_out_parts.append(total.astype(jnp.bfloat16))
    w_out_part = jnp.concatenate(w_out_parts, axis=1)
    moved = lax.all_to_all(w_out_part, PLANE, 0, 0, tiled=True)
    w_out_grad = jnp.sum(
        moved.reshape(plane_count, -1, half_width).astype(jnp.float32), axis=0
    )
    grads = contract(both, preact_grad, 0, 0)
    w_in_part = grads[: feats // 2]
    gain_part = jnp.sum(grads[feats // 2 :] * own_w_in, axis=1)
    b_part = jnp.sum(preact_grad, axis=0, dtype=jnp.float32)
    bias_part = jnp.sum(own_w_in * b_part[None, :], axis=1)
    out_part = jnp.dot(
        mask[:rows].T.astype(jnp.bfloat16), lm, preferred_element_type=jnp.float32
    )[0]
    vectors = jnp.concatenate([gain_part, bias_part, b_part, out_part])
    width = hidden_width // 2
    vector_rows = jnp.concatenate(split_terms(vectors)).reshape(-1, width)
    pieces = w_in_part.astype(jnp.bfloat16).reshape(img_count, piece, 2, width)
    pieces = pieces.transpose(2, 0, 1, 3).reshape(plane_count, piece, width)
    sent = jnp.concatenate(
        [pieces, jnp.broadcast_to(vector_rows, (plane_count, *vector_rows.shape))], axis=1
    )
    moved = lax.all_to_all(sent, PLANE, 0, 0, tiled=True)
    summed = jnp.sum(moved.astype(jnp.float32), axis=0)
    w_in_grad = summed[:piece]
    vectors = summed[piece:].reshape(2, -1).sum(axis=0)
    every = jnp.broadcast_to(vectors, (z_count * 2, vectors.shape[0]))
    every = lax.all_to_all(every, ("z", "c"), 0, 0, tiled=True)
    every = every.reshape(z_count, 2, -1)
    half = feats // 2
    over_z = jnp.sum(every, axis=0)

    def by_core(part):
        return part.reshape(2, img_count, piece).transpose(1, 0, 2).reshape(-1)

    gain_grad = by_core(over_z[:, :half])
    bias_grad = by_core(over_z[:, half : 2 * half])
    b_in_grad = every[:, 0, 2 * half : 2 * half + hidden_width].reshape(-1)
    b_out_grad = over_z[:, 2 * half + hidden_width :].reshape(-1)
    return (w_in_grad, b_in_grad, w_out_grad, b_out_grad, gain_grad, bias_grad)


def solution(mesh):
    finer = Mesh(
        mesh.devices.reshape(8, 2, 4, 2, mesh.shape["fsdp"]),
        ("z", "xl", "y", "xh", "c"),
    )
    placed = (
        P(IMG, ("z", "xl", "c"), None),
        P(),
        P(),
        P("c", SEQ),
        P(SEQ),
        P(SEQ, "c"),
        P(IMG, SEQ, "c"),
        P(IMG, None),
        P(IMG, None),
    )
    return jax.shard_map(
        per_device,
        mesh=finer,
        in_specs=placed,
        out_specs=(P(("y", "xh", "c"), SEQ), P(), P(("z", "xl", "y", "xh"), "c"), P(), P(), P()),
        check_vma=False,
    )
```

```python
import jax
import jax.numpy as jnp
from jax import lax
from jax.experimental import pallas as pl
from jax.experimental.pallas import tpu as pltpu
from jax.sharding import Mesh
from jax.sharding import PartitionSpec as P

PATCH = 576
LEN = 2048
SEQ = ("z", "xl")
IMG = ("y", "xh")
PLANE = ("xl", "y", "xh")


def gelu_parts(preact):
    cumul = 0.5 * (1.0 + lax.erf(preact * 0.7071067811865476))
    density = jnp.exp(-0.5 * preact * preact) * 0.3989422804014327
    return (preact * cumul, cumul + preact * density)


def contract(left, right, left_dim, right_dim):
    return lax.dot_general(
        left, right, (((left_dim,), (right_dim,)), ((), ())), preferred_element_type=jnp.float32
    )


def swap(array, axis):
    return lax.ppermute(array, axis, [(0, 1), (1, 0)])


def in_axis_order(own, other, axis):
    first = lax.axis_index(axis) == 0
    return jnp.where(first, own, other), jnp.where(first, other, own)


def along_z(array, shift):
    count = lax.axis_size("z")
    return lax.ppermute(array, "z", [(i, (i + shift) % count) for i in range(count)])


def gate(*values):
    return lax.optimization_barrier(values)


def whole(shape):
    return pl.BlockSpec(shape, lambda *_: (0,) * len(shape))


def summed_product(left, blocks):
    rows, width = blocks[0].shape
    tile = 256

    def kernel(left_ref, *refs):
        right = jnp.concatenate([ref[...] for ref in refs[:-1]], axis=0)
        total = jnp.dot(left_ref[...], right, preferred_element_type=jnp.float32)
        refs[-1][...] = total.astype(jnp.bfloat16)

    flops = 2 * left.shape[0] * left.shape[1] * width
    return pl.pallas_call(
        kernel,
        grid=(width // tile,),
        in_specs=[whole(left.shape)]
        + [pl.BlockSpec((rows, tile), lambda j: (0, j)) for _ in blocks],
        out_specs=pl.BlockSpec((left.shape[0], tile), lambda j: (0, j)),
        out_shape=jax.ShapeDtypeStruct((left.shape[0], width), jnp.bfloat16),
        cost_estimate=pl.CostEstimate(
            flops=flops,
            bytes_accessed=2 * (left.size + 2 * blocks[0].size * len(blocks)),
            transcendentals=0,
        ),
        name="summed_product",
    )(left, *blocks)


def hidden_products(weights, first, second):
    rows, width = first[0].shape
    count = len(first)
    hidden = weights.shape[0]

    def kernel(w_ref, *refs):
        total_ref, rounded_ref = refs[2 * count :]
        for i in range(count):
            block = jnp.concatenate([refs[i][...], refs[count + i][...]], axis=1)
            total = contract(w_ref[...], block, 1, 1)
            total_ref[:, i * rows : (i + 1) * rows] = total
            rounded_ref[:, i * rows : (i + 1) * rows] = total.astype(jnp.bfloat16)

    out = (hidden, count * rows)
    return pl.pallas_call(
        kernel,
        grid=(1,),
        in_specs=[whole(weights.shape)] + [whole(first[0].shape)] * (2 * count),
        out_specs=[whole(out), whole(out)],
        out_shape=[jax.ShapeDtypeStruct(out, jnp.float32), jax.ShapeDtypeStruct(out, jnp.bfloat16)],
        cost_estimate=pl.CostEstimate(
            flops=4 * count * rows * width * hidden,
            bytes_accessed=4 * count * rows * width,
            transcendentals=0,
        ),
        name="hidden_products",
    )(weights, *first, *second)


def forward(seen, abs_pos, bases, window_starts, image_starts, w_turned, b_column, gain, bias, rows):
    count = bases.shape[0]
    tokens, feats = seen.shape
    hidden = w_turned.shape[0]
    window = 384
    images = image_starts.shape[0]

    def kernel(base_ref, window_ref, image_ref, seen_ref, pos_ref, w_ref, b_ref, gain_ref, bias_ref,
               in_ref, normed_ref, hidden_ref, slope_ref):
        step = pl.program_id(0)
        base = base_ref[step]
        begin = pl.multiple_of(window_ref[step], 128)
        own = base + lax.broadcasted_iota(jnp.int32, (rows, window), 0)
        select = (own == pos_ref[:, pl.ds(begin, window)]).astype(jnp.float32).astype(jnp.bfloat16)
        placed = jnp.dot(
            select, seen_ref[pl.ds(begin, window), :], preferred_element_type=jnp.float32
        )
        mean = jnp.mean(placed, axis=1, keepdims=True)
        centred = placed - mean
        var = jnp.mean(centred * centred, axis=1, keepdims=True)
        normed = centred * lax.rsqrt(var + 1e-05)
        normed_in = (normed * gain_ref[...] + bias_ref[...]).astype(jnp.bfloat16)
        in_ref[...] = normed_in
        normed_ref[...] = normed.astype(jnp.bfloat16)
        preact = contract(w_ref[...], normed_in, 1, 1) + b_ref[...]
        activ, slope = gelu_parts(preact)
        column = base + lax.broadcasted_iota(jnp.int32, (1, rows), 1)
        mask = jnp.zeros((1, rows), jnp.float32)
        for i in range(images):
            start = image_ref[i]
            inside = (column >= start) & (column < start + PATCH)
            mask = jnp.where(inside, 1.0, mask)
        hidden_ref[...] = (activ * mask).astype(jnp.bfloat16)
        slope_ref[...] = slope * mask

    positions = count * rows
    return pl.pallas_call(
        kernel,
        grid_spec=pltpu.PrefetchScalarGridSpec(
            num_scalar_prefetch=3,
            grid=(count,),
            in_specs=[
                whole(seen.shape),
                whole((1, tokens)),
                whole(w_turned.shape),
                whole((hidden, 1)),
                whole((1, feats)),
                whole((1, feats)),
            ],
            out_specs=[
                pl.BlockSpec((rows, feats), lambda i, *_: (i, 0)),
                pl.BlockSpec((rows, feats), lambda i, *_: (i, 0)),
                pl.BlockSpec((hidden, rows), lambda i, *_: (0, i)),
                pl.BlockSpec((hidden, rows), lambda i, *_: (0, i)),
            ],
        ),
        out_shape=[
            jax.ShapeDtypeStruct((positions, feats), jnp.bfloat16),
            jax.ShapeDtypeStruct((positions, feats), jnp.bfloat16),
            jax.ShapeDtypeStruct((hidden, positions), jnp.bfloat16),
            jax.ShapeDtypeStruct((hidden, positions), jnp.float32),
        ],
        cost_estimate=pl.CostEstimate(
            flops=2 * positions * feats * (window + hidden),
            bytes_accessed=20 * positions * hidden,
            transcendentals=2 * positions * hidden,
        ),
        name="forward",
    )(bases, window_starts, image_starts, seen, abs_pos, w_turned, b_column, gain, bias)


TILE = 256


def preact_grads(part_ref, other_ref, slope_ref, held_ref, group, rows):
    for i, block in enumerate(group):
        here = slice(i * rows, (i + 1) * rows)
        total = part_ref[:, here] + other_ref[:, here].astype(jnp.float32)
        total = total * slope_ref[:, block * rows : (block + 1) * rows]
        held_ref[:, here] = total.astype(jnp.bfloat16)


def of_group(ref, group, rows):
    return jnp.concatenate([ref[i * rows : (i + 1) * rows, :] for i in group], axis=0)


def input_products(part, other, slope, normed_in, normed, group, rows):
    hidden, held = part.shape
    positions, feats = normed_in.shape

    def kernel(part_ref, other_ref, slope_ref, in_ref, normed_ref, w_out, g_out, b_out, held_ref):
        @pl.when(pl.program_id(0) == 0)
        def _():
            preact_grads(part_ref, other_ref, slope_ref, held_ref, group, rows)
            ones = jnp.ones((8, held), jnp.bfloat16)
            b_out[...] = contract(ones, held_ref[...], 1, 1)

        grads = held_ref[...]
        w_out[...] = jnp.dot(
            grads, of_group(in_ref, group, rows), preferred_element_type=jnp.float32
        )
        g_out[...] = jnp.dot(
            grads, of_group(normed_ref, group, rows), preferred_element_type=jnp.float32
        )

    column = pl.BlockSpec((positions, TILE), lambda j: (0, j))
    tile = pl.BlockSpec((hidden, TILE), lambda j: (0, j))
    return pl.pallas_call(
        kernel,
        grid=(feats // TILE,),
        in_specs=[whole(part.shape), whole(part.shape), whole(slope.shape), column, column],
        out_specs=[tile, tile, whole((8, hidden))],
        out_shape=[
            jax.ShapeDtypeStruct((hidden, feats), jnp.float32),
            jax.ShapeDtypeStruct((hidden, feats), jnp.float32),
            jax.ShapeDtypeStruct((8, hidden), jnp.float32),
        ],
        scratch_shapes=[pltpu.VMEM((hidden, held), jnp.bfloat16)],
        cost_estimate=pl.CostEstimate(
            flops=4 * held * hidden * feats, bytes_accessed=8 * positions * feats, transcendentals=0
        ),
        name="input_products",
    )(part, other, slope, normed_in, normed)


def input_pieces(part, other, slope, normed_in, normed, before, w_turned, out_rows, core, group, rows, images):
    hidden, held = part.shape
    positions, feats = normed_in.shape
    piece = feats // (images * 2)
    width = hidden // 2
    steps = feats // TILE
    per_step = images // steps
    gain_rows, b_rows = steps, hidden // TILE
    total_rows = 2 * gain_rows + b_rows + out_rows.shape[0]
    padded = -(-total_rows // 8) * 8

    def kernel(core_ref, part_ref, other_ref, slope_ref, in_ref, normed_ref, w_before, g_before, b_before,
               w_ref, rows_ref, sent_ref, held_ref, turned_ref, vector_ref, column_ref):
        step = pl.program_id(0)

        @pl.when(step == 0)
        def _():
            preact_grads(part_ref, other_ref, slope_ref, held_ref, group, rows)
            ones = jnp.ones((8, held), jnp.bfloat16)
            sums = contract(ones, held_ref[...], 1, 1) + b_before[...]
            vector_ref[...] = jnp.zeros_like(vector_ref)
            for i in range(b_rows):
                vector_ref[2 * gain_rows + i : 2 * gain_rows + i + 1, :] = sums[
                    0:1, i * TILE : (i + 1) * TILE
                ]
            first = 2 * gain_rows + b_rows
            vector_ref[first : first + rows_ref.shape[0], :] = rows_ref[...]
            column_ref[...] = jnp.broadcast_to(sums[0:1, :], (128, hidden)).T

        grads = held_ref[...]
        w_grad = w_before[...] + jnp.dot(
            grads, of_group(in_ref, group, rows), preferred_element_type=jnp.float32
        )
        g_grad = g_before[...] + jnp.dot(
            grads, of_group(normed_ref, group, rows), preferred_element_type=jnp.float32
        )
        turned_ref[...] = w_grad.T
        for i in range(per_step):
            own = pl.multiple_of(i * 2 * piece + core_ref[0] * piece, piece)
            for half in range(2):
                sent_ref[half * images + step * per_step + i, 0:piece, :] = turned_ref[
                    pl.ds(own, piece), half * width : (half + 1) * width
                ].astype(jnp.bfloat16)
        weights = w_ref[...].astype(jnp.float32)
        column = jnp.concatenate([column_ref[...]] * (TILE // 128), axis=1)
        vector_ref[pl.ds(step, 1), :] = jnp.sum(g_grad * weights, axis=0, keepdims=True)
        vector_ref[pl.ds(gain_rows + step, 1), :] = jnp.sum(column * weights, axis=0, keepdims=True)

        @pl.when(step == steps - 1)
        def _():
            vectors = vector_ref[...]
            high = vectors.astype(jnp.bfloat16).astype(jnp.float32)
            both = jnp.concatenate([high, vectors - high], axis=0).astype(jnp.bfloat16)
            for i in range(2 * images):
                sent_ref[i, piece : piece + 2 * padded, :] = both

    column = pl.BlockSpec((positions, TILE), lambda j, *_: (0, j))
    tile = pl.BlockSpec((hidden, TILE), lambda j, *_: (0, j))
    sent = (2 * images, piece + 2 * padded, width)
    return pl.pallas_call(
        kernel,
        grid_spec=pltpu.PrefetchScalarGridSpec(
            num_scalar_prefetch=1,
            grid=(steps,),
            in_specs=[
                whole(part.shape),
                whole(part.shape),
                whole(slope.shape),
                column,
                column,
                tile,
                tile,
                whole((8, hidden)),
                tile,
                whole(out_rows.shape),
            ],
            out_specs=whole(sent),
            scratch_shapes=[
                pltpu.VMEM((hidden, held), jnp.bfloat16),
                pltpu.VMEM((TILE, hidden), jnp.float32),
                pltpu.VMEM((padded, TILE), jnp.float32),
                pltpu.VMEM((hidden, 128), jnp.float32),
            ],
        ),
        out_shape=jax.ShapeDtypeStruct(sent, jnp.bfloat16),
        cost_estimate=pl.CostEstimate(
            flops=4 * held * hidden * feats, bytes_accessed=8 * positions * feats, transcendentals=0
        ),
        name="input_pieces",
    )(core, part, other, slope, normed_in, normed, *before, w_turned, out_rows)


def split_terms(vector):
    high = vector.astype(jnp.bfloat16)
    low = (vector - high.astype(jnp.float32)).astype(jnp.bfloat16)
    return high, low


def per_device(vision_feats, ln_gain, ln_bias, w_in, b_in, w_out, lm_grad, image_counts, token_pos):
    z_count = lax.axis_size("z")
    z = lax.axis_index("z")
    xl = lax.axis_index("xl")
    core = lax.axis_index("c")
    vision = vision_feats[0]
    lm = lm_grad[0]
    rows, half_width = lm.shape
    feats = vision.shape[1]
    quarter = half_width // 2
    counts = image_counts[0]
    positions = token_pos[0]
    tokens = positions.shape[0]
    image_index = jnp.arange(tokens, dtype=jnp.int32) // PATCH
    abs_pos = jnp.where(image_index >= counts[0], LEN, 0) + positions
    copies = jnp.broadcast_to(vision, (z_count, *vision.shape))
    seen = lax.all_to_all(copies, "z", 0, 0, tiled=True)
    low, high = [None] * z_count, [None] * z_count
    low[0] = lm[:, :quarter]
    low[7], low[1] = along_z(low[0], 1), along_z(low[0], -1)
    w_out_other = swap(w_out, "xl")
    terms = split_terms(b_in)
    third = (b_in - terms[0].astype(jnp.float32) - terms[1].astype(jnp.float32)).astype(jnp.bfloat16)
    w_first, w_second = in_axis_order(w_in, swap(w_in, "c"), "c")
    packed = jnp.concatenate(
        [w_first, w_second, jnp.stack([*terms, third]), jnp.zeros((5, b_in.shape[0]), jnp.bfloat16)]
    )
    packed_other = swap(packed, "xl")
    hidden_width = 2 * w_out.shape[0]
    block_of = lax.rem(z + jnp.arange(z_count, dtype=jnp.int32), z_count)
    bases = (2 * block_of + xl) * rows
    image_starts = abs_pos[::PATCH]
    first_token = jnp.sum((abs_pos[None, :] < bases[:, None]).astype(jnp.int32), axis=1)
    window_starts = jnp.minimum(first_token // 128 * 128, tokens - 384)
    own_pos = bases[0] + jnp.arange(rows, dtype=jnp.int32)
    inside = (own_pos[:, None] >= image_starts) & (own_pos[:, None] < image_starts + PATCH)
    mask = jnp.any(inside, axis=1).astype(jnp.bfloat16)
    out_part = jnp.dot(mask[None, :], lm, preferred_element_type=jnp.float32).reshape(-1, TILE)
    seen, low[7], low[1], high[0] = gate(seen, low[7], low[1], lm[:, quarter:])
    low[6], low[2] = along_z(low[7], 1), along_z(low[1], -1)
    high[7], high[1] = along_z(high[0], 1), along_z(high[0], -1)
    seen_other = swap(seen, "xl")
    low[6], low[2], packed, packed_other, w_out_other, out_part = gate(
        low[6], low[2], packed, packed_other, w_out_other, out_part
    )
    low[5], low[3] = along_z(low[6], 1), along_z(low[2], -1)
    packed = jnp.concatenate(in_axis_order(packed, packed_other, "xl"), axis=1)
    w_turned = packed[:feats].T
    b_column = jnp.sum(packed[feats : feats + 3].astype(jnp.float32), axis=0)[:, None]
    w_out_all = jnp.concatenate(in_axis_order(w_out, w_out_other, "xl"), axis=0)
    high[7], high[1], seen_other, w_turned, b_column, w_out_all = gate(
        high[7], high[1], seen_other, w_turned, b_column, w_out_all
    )
    high[6], high[2] = along_z(high[7], 1), along_z(high[1], -1)
    seen = jnp.stack(in_axis_order(seen, seen_other, "xl"), axis=1)
    seen_other = swap(seen, "c")
    low[5], low[3], seen_other = gate(low[5], low[3], seen_other)
    low[4] = along_z(low[5], 1)
    seen = jnp.stack(in_axis_order(seen, seen_other, "c"), axis=2).reshape(tokens, feats)
    normed_in, normed, hidden, slope = forward(
        seen,
        abs_pos[None, :],
        bases,
        window_starts,
        image_starts,
        w_turned,
        b_column,
        ln_gain[None, :],
        ln_bias[None, :],
        rows,
    )
    high[6], high[2], normed_in, normed, hidden, slope = gate(
        high[6], high[2], normed_in, normed, hidden, slope
    )
    high[5], high[3] = along_z(high[6], 1), along_z(high[2], -1)
    early, late = (6, 7, 0, 1, 2), (3, 4, 5)
    part, rounded = hidden_products(w_out_all, [low[i] for i in early], [high[i] for i in early])
    low[4], high[3], part, rounded = gate(low[4], high[3], part, rounded)
    high[4] = along_z(high[3], -1)
    other = swap(rounded, "c")
    low_product = summed_product(hidden, low)
    low_product, normed_in, normed, slope = gate(low_product, normed_in, normed, slope)
    low_moved = lax.all_to_all(low_product, PLANE, 0, 0, tiled=True)
    before = input_products(part, other, slope, normed_in, normed, early, rows)
    high[4], high[5], *before = gate(high[4], high[5], *before)
    part, rounded = hidden_products(w_out_all, [low[i] for i in late], [high[i] for i in late])
    other = swap(rounded, "c")
    high_product = summed_product(hidden, high)
    plane_count = lax.axis_size(PLANE)
    img_count = lax.axis_size(IMG)
    piece = feats // (img_count * 2)
    sent = input_pieces(
        part,
        other,
        slope,
        normed_in,
        normed,
        before,
        w_turned,
        out_part,
        core.reshape(1),
        late,
        rows,
        img_count,
    )
    sent, low_moved = gate(sent, low_moved)
    moved = lax.all_to_all(sent, PLANE, 0, 0, tiled=True)
    moved, high_product = gate(moved, high_product)
    high_moved = lax.all_to_all(high_product, PLANE, 0, 0, tiled=True)
    summed = jnp.sum(moved.astype(jnp.float32), axis=0)
    w_in_grad = summed[:piece]
    padded = (summed.shape[0] - piece) // 2
    vectors = summed[piece : piece + padded] + summed[piece + padded :]
    line = feats // TILE
    b_lines = hidden_width // TILE
    out_lines = half_width // TILE
    b_own = vectors[2 * line : 2 * line + b_lines]
    b_full = jnp.where((jnp.arange(z_count) == z)[:, None, None], b_own[None], 0.0)
    vectors = jnp.concatenate(
        [
            vectors[: 2 * line],
            vectors[2 * line + b_lines : 2 * line + b_lines + out_lines],
            b_full.reshape(-1, TILE),
        ]
    )
    for shift in (1, 2, 4):
        vectors = vectors + lax.ppermute(vectors, "z", [(i, i ^ shift) for i in range(z_count)])
    first, second = in_axis_order(vectors, swap(vectors, "c"), "c")
    gain_grad = first[:line].reshape(-1)
    bias_grad = first[line : 2 * line].reshape(-1)
    out_end = 2 * line + out_lines
    b_out_grad = jnp.concatenate([first[2 * line : out_end], second[2 * line : out_end]]).reshape(-1)
    b_in_grad = first[out_end:].reshape(-1)

    def over_plane(array):
        return jnp.sum(array.reshape(plane_count, -1, quarter).astype(jnp.float32), axis=0)

    w_out_grad = jnp.concatenate([over_plane(low_moved), over_plane(high_moved)], axis=1)
    return (w_in_grad, b_in_grad, w_out_grad, b_out_grad, gain_grad, bias_grad)


def solution(mesh):
    finer = Mesh(
        mesh.devices.reshape(8, 2, 4, 2, mesh.shape["fsdp"]),
        ("z", "xl", "y", "xh", "c"),
    )
    placed = (
        P(IMG, ("z", "xl", "c"), None),
        P(),
        P(),
        P("c", SEQ),
        P(SEQ),
        P(SEQ, "c"),
        P(IMG, SEQ, "c"),
        P(IMG, None),
        P(IMG, None),
    )
    return jax.shard_map(
        per_device,
        mesh=finer,
        in_specs=placed,
        out_specs=(P(("y", "xh", "c"), SEQ), P(), P(("z", "xl", "y", "xh"), "c"), P(), P(), P()),
        check_vma=False,
    )
```

```python
import jax
import jax.numpy as jnp
from jax import lax
from jax.experimental import pallas as pl
from jax.experimental.pallas import tpu as pltpu
from jax.sharding import Mesh
from jax.sharding import PartitionSpec as P

PATCH = 576
LEN = 2048
SEQ = ("z", "xl")
IMG = ("y", "xh")
PLANE = ("xl", "y", "xh")


def gelu_parts(preact):
    cumul = 0.5 * (1.0 + lax.erf(preact * 0.7071067811865476))
    density = jnp.exp(-0.5 * preact * preact) * 0.3989422804014327
    return (preact * cumul, cumul + preact * density)


def contract(left, right, left_dim, right_dim):
    return lax.dot_general(
        left, right, (((left_dim,), (right_dim,)), ((), ())), preferred_element_type=jnp.float32
    )


def swap(array, axis):
    return lax.ppermute(array, axis, [(0, 1), (1, 0)])


def in_axis_order(own, other, axis):
    first = lax.axis_index(axis) == 0
    return jnp.where(first, own, other), jnp.where(first, other, own)


def along_z(array, shift):
    count = lax.axis_size("z")
    return lax.ppermute(array, "z", [(i, (i + shift) % count) for i in range(count)])


def gate(*values):
    return lax.optimization_barrier(values)


def whole(shape):
    return pl.BlockSpec(shape, lambda *_: (0,) * len(shape))


def summed_product(left, blocks):
    rows, width = blocks[0].shape
    tile = width // 2

    def kernel(left_ref, *refs):
        right = jnp.concatenate([ref[...] for ref in refs[:-1]], axis=0)
        total = jnp.dot(left_ref[...], right, preferred_element_type=jnp.float32)
        refs[-1][...] = total.astype(jnp.bfloat16)

    flops = 2 * left.shape[0] * left.shape[1] * width
    return pl.pallas_call(
        kernel,
        grid=(width // tile,),
        in_specs=[whole(left.shape)]
        + [pl.BlockSpec((rows, tile), lambda j: (0, j)) for _ in blocks],
        out_specs=pl.BlockSpec((left.shape[0], tile), lambda j: (0, j)),
        out_shape=jax.ShapeDtypeStruct((left.shape[0], width), jnp.bfloat16),
        cost_estimate=pl.CostEstimate(
            flops=flops,
            bytes_accessed=2 * (left.size + 2 * blocks[0].size * len(blocks)),
            transcendentals=0,
        ),
        name="summed_product",
    )(left, *blocks)


def hidden_products(weights, place, first, second):
    rows, width = first[0].shape
    count = len(first)
    hidden = weights[0].shape[0]

    def kernel(place_ref, own_ref, other_ref, *refs):
        total_ref, rounded_ref = refs[2 * count :]
        spots = (place_ref[0], 1 - place_ref[0])
        for i in range(count):
            block = jnp.concatenate([refs[i][...], refs[count + i][...]], axis=1)
            for ref, spot in zip((own_ref, other_ref), spots):
                total = contract(ref[...], block, 1, 1)
                here = pl.ds(pl.multiple_of(spot * hidden, hidden), hidden)
                total_ref[here, i * rows : (i + 1) * rows] = total
                rounded_ref[here, i * rows : (i + 1) * rows] = total.astype(jnp.bfloat16)

    out = (2 * hidden, count * rows)
    return pl.pallas_call(
        kernel,
        grid_spec=pltpu.PrefetchScalarGridSpec(
            num_scalar_prefetch=1,
            grid=(1,),
            in_specs=[whole(weights[0].shape)] * 2 + [whole(first[0].shape)] * (2 * count),
            out_specs=[whole(out), whole(out)],
        ),
        out_shape=[jax.ShapeDtypeStruct(out, jnp.float32), jax.ShapeDtypeStruct(out, jnp.bfloat16)],
        cost_estimate=pl.CostEstimate(
            flops=8 * count * rows * width * hidden,
            bytes_accessed=4 * count * rows * width,
            transcendentals=0,
        ),
        name="hidden_products",
    )(place, *weights, *first, *second)


def forward(
    seen, held_pos, bases, window_starts, image_starts, w_turned, b_column, gain, bias, core, rows, piece
):
    count = bases.shape[0]
    _, window, feats = seen.shape
    window = 2 * window
    hidden = w_turned.shape[0]
    images = image_starts.shape[0]

    def own_half(array, core):
        lane = lax.broadcasted_iota(jnp.int32, (rows, 2 * piece), 1)
        first = core == 0
        kept = (lane < piece) == first
        held = []
        for i in range(0, feats, 4 * piece):
            left, right = array[:, i : i + 2 * piece], array[:, i + 2 * piece : i + 4 * piece]
            turned = pltpu.roll(jnp.where(first, right, left), piece, 1)
            held.append(jnp.where(kept, jnp.where(first, left, right), turned))
        return jnp.concatenate(held, axis=1)

    def kernel(base_ref, window_ref, image_ref, core_ref, seen_ref, pos_ref, w_ref, b_ref, gain_ref, bias_ref, own_gain_ref, own_bias_ref,
               in_ref, normed_ref, hidden_ref, slope_ref):
        step = pl.program_id(0)
        base = base_ref[step]
        begin = window_ref[step]
        own = base + lax.broadcasted_iota(jnp.int32, (rows, window), 0)
        select = (own == pos_ref[begin]).astype(jnp.float32).astype(jnp.bfloat16)
        held = seen_ref[pl.ds(begin, 2)].reshape(window, feats)
        placed = jnp.dot(select, held, preferred_element_type=jnp.float32)
        mean = jnp.mean(placed, axis=1, keepdims=True)
        centred = placed - mean
        var = jnp.mean(centred * centred, axis=1, keepdims=True)
        normed = centred * lax.rsqrt(var + 1e-05)
        normed_in = (normed * gain_ref[...] + bias_ref[...]).astype(jnp.bfloat16)
        own_normed = own_half(normed, core_ref[0])
        in_ref[...] = (own_normed * own_gain_ref[...] + own_bias_ref[...]).astype(jnp.bfloat16)
        normed_ref[...] = own_normed.astype(jnp.bfloat16)
        preact = contract(w_ref[...], normed_in, 1, 1) + b_ref[...]
        activ, slope = gelu_parts(preact)
        column = base + lax.broadcasted_iota(jnp.int32, (1, rows), 1)
        mask = jnp.zeros((1, rows), jnp.float32)
        for i in range(images):
            start = image_ref[i]
            inside = (column >= start) & (column < start + PATCH)
            mask = jnp.where(inside, 1.0, mask)
        hidden_ref[...] = (activ * mask).astype(jnp.bfloat16)
        slope_ref[...] = slope * mask

    positions = count * rows
    return pl.pallas_call(
        kernel,
        grid_spec=pltpu.PrefetchScalarGridSpec(
            num_scalar_prefetch=4,
            grid=(count,),
            in_specs=[
                whole(seen.shape),
                whole(held_pos.shape),
                whole(w_turned.shape),
                whole((hidden, 1)),
                whole((1, feats)),
                whole((1, feats)),
                whole((1, feats // 2)),
                whole((1, feats // 2)),
            ],
            out_specs=[
                pl.BlockSpec((rows, feats // 2), lambda i, *_: (i, 0)),
                pl.BlockSpec((rows, feats // 2), lambda i, *_: (i, 0)),
                pl.BlockSpec((hidden, rows), lambda i, *_: (0, i)),
                pl.BlockSpec((hidden, rows), lambda i, *_: (0, i)),
            ],
        ),
        out_shape=[
            jax.ShapeDtypeStruct((positions, feats // 2), jnp.bfloat16),
            jax.ShapeDtypeStruct((positions, feats // 2), jnp.bfloat16),
            jax.ShapeDtypeStruct((hidden, positions), jnp.bfloat16),
            jax.ShapeDtypeStruct((hidden, positions), jnp.float32),
        ],
        cost_estimate=pl.CostEstimate(
            flops=2 * positions * feats * (window + hidden),
            bytes_accessed=20 * positions * hidden,
            transcendentals=2 * positions * hidden,
        ),
        name="forward",
    )(bases, window_starts, image_starts, core, seen, held_pos, w_turned, b_column, gain[0], bias[0], gain[1], bias[1])


TILE = 256


def preact_grads(parts, others, slope_ref, held_ref, groups, rows):
    at = 0
    for part, other, group in zip(parts, others, groups):
        for i, block in enumerate(group):
            here = slice(i * rows, (i + 1) * rows)
            total = part[:, here] + other[:, here].astype(jnp.float32)
            total = total * slope_ref[:, block * rows : (block + 1) * rows]
            held_ref[:, at * rows : (at + 1) * rows] = total.astype(jnp.bfloat16)
            at += 1


def of_groups(ref, groups, rows):
    return jnp.concatenate(
        [ref[i * rows : (i + 1) * rows, :] for group in groups for i in group], axis=0
    )


def input_products(parts, others, slope, normed_in, normed, groups, rows):
    count = len(groups)
    hidden = slope.shape[0]
    held = rows * sum(len(group) for group in groups)
    positions, feats = normed_in.shape

    def kernel(*refs):
        parts, others = refs[:count], refs[count : 2 * count]
        slope_ref, in_ref, normed_ref, w_out, g_out, b_out, held_ref = refs[2 * count :]

        @pl.when(pl.program_id(0) == 0)
        def _():
            preact_grads(parts, others, slope_ref, held_ref, groups, rows)
            ones = jnp.ones((8, held), jnp.bfloat16)
            b_out[...] = contract(ones, held_ref[...], 1, 1)

        grads = held_ref[...]
        w_out[...] = jnp.dot(
            grads, of_groups(in_ref, groups, rows), preferred_element_type=jnp.float32
        )
        g_out[...] = jnp.dot(
            grads, of_groups(normed_ref, groups, rows), preferred_element_type=jnp.float32
        )

    column = pl.BlockSpec((positions, TILE), lambda j: (0, j))
    tile = pl.BlockSpec((hidden, TILE), lambda j: (0, j))
    return pl.pallas_call(
        kernel,
        grid=(feats // TILE,),
        in_specs=[whole(a.shape) for a in (*parts, *others)] + [whole(slope.shape), column, column],
        out_specs=[tile, tile, whole((8, hidden))],
        out_shape=[
            jax.ShapeDtypeStruct((hidden, feats), jnp.float32),
            jax.ShapeDtypeStruct((hidden, feats), jnp.float32),
            jax.ShapeDtypeStruct((8, hidden), jnp.float32),
        ],
        scratch_shapes=[pltpu.VMEM((hidden, held), jnp.bfloat16)],
        cost_estimate=pl.CostEstimate(
            flops=4 * held * hidden * feats, bytes_accessed=8 * positions * feats, transcendentals=0
        ),
        name="input_products",
    )(*parts, *others, slope, normed_in, normed)


def input_pieces(part, other, slope, normed_in, normed, before, w_own, out_rows, rows, at, images):
    hidden, held = part.shape
    own_feats = normed_in.shape[1]
    piece = own_feats // images
    width = hidden // 2
    steps = own_feats // TILE
    per_step = images // steps
    b_rows = hidden // TILE
    total_rows = 2 * steps + b_rows + out_rows.shape[0]
    padded = -(-total_rows // 8) * 8

    def kernel(part_ref, other_ref, slope_ref, in_ref, normed_ref, w_before, g_before, b_before,
               w_ref, rows_ref, sent_ref, held_ref, vector_ref, column_ref):
        step = pl.program_id(0)

        @pl.when(step == 0)
        def _():
            preact_grads([part_ref], [other_ref], slope_ref, held_ref, [range(held // rows)], rows)
            ones = jnp.ones((8, held), jnp.bfloat16)
            sums = contract(ones, held_ref[...], 1, 1) + b_before[...]
            vector_ref[...] = jnp.zeros_like(vector_ref)
            for i in range(b_rows):
                vector_ref[2 * steps + i : 2 * steps + i + 1, :] = sums[
                    0:1, i * TILE : (i + 1) * TILE
                ]
            first = 2 * steps + b_rows
            vector_ref[first : first + rows_ref.shape[0], :] = rows_ref[...]
            column_ref[...] = jnp.broadcast_to(sums[0:1, :], (128, hidden)).T

        grads = held_ref[...]
        w_grad = w_before[...] + jnp.dot(grads, in_ref[...], preferred_element_type=jnp.float32)
        g_grad = g_before[...] + jnp.dot(grads, normed_ref[...], preferred_element_type=jnp.float32)
        turned = w_grad.T.astype(jnp.bfloat16)
        for i in range(per_step):
            for half in range(2):
                sent_ref[half * images + step * per_step + i, 0:piece, :] = turned[
                    i * piece : (i + 1) * piece, half * width : (half + 1) * width
                ]
        weights = w_ref[...].astype(jnp.float32)
        column = jnp.concatenate([column_ref[...]] * (TILE // 128), axis=1)
        vector_ref[pl.ds(step, 1), :] = jnp.sum(g_grad * weights, axis=0, keepdims=True)
        vector_ref[pl.ds(steps + step, 1), :] = jnp.sum(column * weights, axis=0, keepdims=True)

        @pl.when(step == steps - 1)
        def _():
            vectors = vector_ref[...]
            high = vectors.astype(jnp.bfloat16).astype(jnp.float32)
            both = jnp.concatenate([high, vectors - high], axis=0).astype(jnp.bfloat16)
            for i in range(2 * images):
                sent_ref[i, piece : piece + 2 * padded, :] = both

    column = pl.BlockSpec((held, TILE), lambda j: (at, j))
    tile = pl.BlockSpec((hidden, TILE), lambda j: (0, j))
    sent = (2 * images, piece + 2 * padded, width)
    return pl.pallas_call(
        kernel,
        grid=(steps,),
        in_specs=[
            whole(part.shape),
            whole(part.shape),
            pl.BlockSpec((hidden, held), lambda j: (0, at)),
            column,
            column,
            tile,
            tile,
            whole((8, hidden)),
            tile,
            whole(out_rows.shape),
        ],
        out_specs=whole(sent),
        scratch_shapes=[
            pltpu.VMEM((hidden, held), jnp.bfloat16),
            pltpu.VMEM((padded, TILE), jnp.float32),
            pltpu.VMEM((hidden, 128), jnp.float32),
        ],
        out_shape=jax.ShapeDtypeStruct(sent, jnp.bfloat16),
        cost_estimate=pl.CostEstimate(
            flops=4 * held * hidden * own_feats, bytes_accessed=8 * held * own_feats, transcendentals=0
        ),
        name="input_pieces",
    )(part, other, slope, normed_in, normed, *before, w_own, out_rows)


def split_terms(vector):
    high = vector.astype(jnp.bfloat16)
    low = (vector - high.astype(jnp.float32)).astype(jnp.bfloat16)
    return high, low


def one_step(vision_feats, ln_gain, ln_bias, w_in, b_in, w_out, lm_grad, image_counts, token_pos):
    z_count = lax.axis_size("z")
    z = lax.axis_index("z")
    xl = lax.axis_index("xl")
    core = lax.axis_index("c")
    vision = vision_feats[0]
    lm = lm_grad[0]
    rows, half_width = lm.shape
    feats = vision.shape[1]
    quarter = half_width // 2
    counts = image_counts[0]
    positions = token_pos[0]
    tokens = positions.shape[0]
    image_index = jnp.arange(tokens, dtype=jnp.int32) // PATCH
    abs_pos = jnp.where(image_index >= counts[0], LEN, 0) + positions
    copies = jnp.broadcast_to(vision, (z_count, *vision.shape))
    seen = lax.all_to_all(copies, "z", 0, 0, tiled=True)
    low, high = [None] * z_count, [None] * z_count
    low[0], high[0] = lm[:, :quarter], lm[:, quarter:]
    low[7], low[1] = along_z(low[0], 1), along_z(low[0], -1)
    high[7], high[1] = along_z(high[0], 1), along_z(high[0], -1)
    w_out_other = swap(w_out, "xl")
    terms = split_terms(b_in)
    third = (b_in - terms[0].astype(jnp.float32) - terms[1].astype(jnp.float32)).astype(jnp.bfloat16)
    w_in_other = swap(w_in, "c")
    w_first, w_second = in_axis_order(w_in, w_in_other, "c")
    packed = jnp.concatenate(
        [w_first, w_second, jnp.stack([*terms, third]), jnp.zeros((5, b_in.shape[0]), jnp.bfloat16)]
    )
    packed_other = swap(packed, "xl")
    hidden_width = 2 * w_out.shape[0]
    plane_count = lax.axis_size(PLANE)
    img_count = lax.axis_size(IMG)
    piece = feats // (img_count * 2)
    packed = jnp.concatenate(in_axis_order(packed, packed_other, "xl"), axis=1)
    w_turned = packed[:feats].T
    w_own = packed[:feats].reshape(img_count, 2, piece, hidden_width)
    w_own = lax.dynamic_index_in_dim(w_own, core, 1, False).reshape(feats // 2, hidden_width).T
    b_column = jnp.sum(packed[feats : feats + 3].astype(jnp.float32), axis=0)[:, None]
    block_of = lax.rem(z + jnp.arange(z_count, dtype=jnp.int32), z_count)
    bases = (2 * block_of + xl) * rows
    image_starts = abs_pos[::PATCH]
    first_token = jnp.sum((abs_pos[None, :] < bases[:, None]).astype(jnp.int32), axis=1)
    of_z = tokens // z_count
    window_starts = jnp.minimum(first_token // of_z, z_count - 2)
    held_pos = abs_pos.reshape(z_count, 2, 2, of_z // 4)
    held_pos = jnp.where(xl == 0, held_pos, held_pos[:, ::-1])
    held_pos = jnp.where(core == 0, held_pos, held_pos[:, :, ::-1])
    held_pos = held_pos.transpose(0, 2, 1, 3).reshape(z_count, 1, of_z)
    own_pos = bases[0] + jnp.arange(rows, dtype=jnp.int32)
    inside = (own_pos[:, None] >= image_starts) & (own_pos[:, None] < image_starts + PATCH)
    mask = jnp.any(inside, axis=1).astype(jnp.bfloat16)
    out_part = jnp.dot(mask[None, :], lm, preferred_element_type=jnp.float32).reshape(-1, TILE)
    held_pos = jnp.concatenate([held_pos[:-1], held_pos[1:]], axis=2)

    def own_part(vector):
        parts = vector.reshape(img_count, 2, piece)
        return lax.dynamic_index_in_dim(parts, core, 1, False).reshape(1, -1)

    seen, w_turned, w_own, b_column, out_part, held_pos = gate(
        seen, w_turned, w_own, b_column, out_part, held_pos
    )
    seen_other = swap(seen, "xl")
    low[7], low[1] = gate(low[7], low[1])
    low[6], low[2] = along_z(low[7], 1), along_z(low[1], -1)
    high[7], high[1] = gate(high[7], high[1])
    high[6], high[2] = along_z(high[7], 1), along_z(high[1], -1)
    weights, place = (w_out, w_out_other), xl.reshape(1)

    def products(blocks):
        return hidden_products(weights, place, [low[i] for i in blocks], [high[i] for i in blocks])

    groups = [(7, 0, 1), (6, 2), (5, 3)]
    parts, others = [None] * 3, [None] * 3
    parts[0], rounded = products(groups[0])
    parts[0], rounded, seen_other = gate(parts[0], rounded, seen_other)
    seen = jnp.stack([seen, seen_other], axis=1)
    seen_other = swap(seen, "c")
    others[0] = swap(rounded, "c")
    low[6], low[2], rounded = gate(low[6], low[2], rounded)
    low[5], low[3] = along_z(low[6], 1), along_z(low[2], -1)
    seen = jnp.stack([seen, seen_other], axis=1).reshape(z_count, of_z, feats)
    normed_in, normed, hidden, slope = forward(
        seen,
        held_pos,
        bases,
        window_starts,
        image_starts,
        w_turned,
        b_column,
        (ln_gain[None, :], own_part(ln_gain)),
        (ln_bias[None, :], own_part(ln_bias)),
        core.reshape(1),
        rows,
        piece,
    )
    high[6], high[2], hidden, others[0] = gate(high[6], high[2], hidden, others[0])
    high[5], high[3] = along_z(high[6], 1), along_z(high[2], -1)
    low[5], low[3], hidden = gate(low[5], low[3], hidden)
    low[4] = along_z(low[5], 1)
    parts[1], rounded = products(groups[1])
    others[1] = swap(rounded, "c")
    high[5], high[3], parts[1] = gate(high[5], high[3], parts[1])
    high[4] = along_z(high[3], -1)
    parts[2], rounded = products(groups[2])
    others[2] = swap(rounded, "c")
    low[4], hidden, parts[2], rounded = gate(low[4], hidden, parts[2], rounded)
    low_product = summed_product(hidden, low)
    low_product, normed_in, normed, slope = gate(low_product, normed_in, normed, slope)
    low_moved = lax.all_to_all(low_product, PLANE, 0, 0, tiled=True)
    before = input_products(parts, others, slope, normed_in, normed, groups, rows)
    high[4], *before = gate(high[4], *before)
    part, rounded = products((4,))
    other = swap(rounded, "c")
    high_product = summed_product(hidden, high)
    sent = input_pieces(
        part, other, slope, normed_in, normed, before, w_own, out_part, rows, 4, img_count
    )
    sent, low_moved = gate(sent, low_moved)
    moved = lax.all_to_all(sent, PLANE, 0, 0, tiled=True)
    moved, high_product = gate(moved, high_product)
    high_moved = lax.all_to_all(high_product, PLANE, 0, 0, tiled=True)
    summed = jnp.sum(moved.astype(jnp.float32), axis=0)
    w_in_grad = summed[:piece]
    padded = (summed.shape[0] - piece) // 2
    vectors = summed[piece : piece + padded] + summed[piece + padded :]
    line = feats // 2 // TILE
    b_lines = hidden_width // TILE
    out_lines = half_width // TILE
    b_own = vectors[2 * line : 2 * line + b_lines]
    b_full = jnp.where((jnp.arange(z_count) == z)[:, None, None], b_own[None], 0.0)
    vectors = jnp.concatenate(
        [
            vectors[: 2 * line],
            vectors[2 * line + b_lines : 2 * line + b_lines + out_lines],
            b_full.reshape(-1, TILE),
        ]
    )
    for shift in (1, 2, 4):
        moved = lax.ppermute(vectors, "z", [(i, i ^ shift) for i in range(z_count)])
        vectors = vectors + moved
    first, second = in_axis_order(vectors, swap(vectors, "c"), "c")

    def by_core(low_half, high_half):
        return jnp.stack([low_half.reshape(-1, piece), high_half.reshape(-1, piece)], 1).reshape(-1)

    gain_grad = by_core(first[:line], second[:line])
    bias_grad = by_core(first[line : 2 * line], second[line : 2 * line])
    out_end = 2 * line + out_lines
    b_out_grad = jnp.concatenate([first[2 * line : out_end], second[2 * line : out_end]]).reshape(-1)
    b_in_grad = first[out_end:].reshape(-1)

    def over_plane(array):
        return jnp.sum(array.reshape(plane_count, -1, quarter).astype(jnp.float32), axis=0)

    w_out_grad = jnp.concatenate([over_plane(low_moved), over_plane(high_moved)], axis=1)
    return (w_in_grad, b_in_grad, w_out_grad, b_out_grad, gain_grad, bias_grad)


def solution(mesh):
    finer = Mesh(
        mesh.devices.reshape(8, 2, 4, 2, mesh.shape["fsdp"]),
        ("z", "xl", "y", "xh", "c"),
    )
    placed = (
        P(IMG, ("z", "xl", "c"), None),
        P(),
        P(),
        P("c", SEQ),
        P(SEQ),
        P(SEQ, "c"),
        P(IMG, SEQ, "c"),
        P(IMG, None),
        P(IMG, None),
    )

    return jax.shard_map(
        one_step,
        mesh=finer,
        in_specs=placed,
        out_specs=(P(("y", "xh", "c"), SEQ), P(), P(("z", "xl", "y", "xh"), "c"), P(), P(), P()),
        check_vma=False,
    )
```

```python
import jax
import jax.numpy as jnp
from jax import lax
from jax.experimental import pallas as pl
from jax.experimental.pallas import tpu as pltpu
from jax.sharding import Mesh
from jax.sharding import PartitionSpec as P

PATCH = 576
LEN = 2048
SEQ = ("z", "xl")
IMG = ("y", "xh")
PLANE = ("xl", "y", "xh")


def gelu_parts(preact):
    cumul = 0.5 * (1.0 + lax.erf(preact * 0.7071067811865476))
    density = jnp.exp(-0.5 * preact * preact) * 0.3989422804014327
    return (preact * cumul, cumul + preact * density)


def contract(left, right, left_dim, right_dim):
    return lax.dot_general(
        left, right, (((left_dim,), (right_dim,)), ((), ())), preferred_element_type=jnp.float32
    )


def swap(array, axis):
    return lax.ppermute(array, axis, [(0, 1), (1, 0)])


def in_axis_order(own, other, axis):
    first = lax.axis_index(axis) == 0
    return jnp.where(first, own, other), jnp.where(first, other, own)


def along_z(array, shift):
    count = lax.axis_size("z")
    return lax.ppermute(array, "z", [(i, (i + shift) % count) for i in range(count)])


def gate(*values):
    return lax.optimization_barrier(values)


def whole(shape):
    return pl.BlockSpec(shape, lambda *_: (0,) * len(shape))


def summed_product(left, blocks):
    rows, width = blocks[0].shape
    tile = width // 2

    def kernel(left_ref, *refs):
        right = jnp.concatenate([ref[...] for ref in refs[:-1]], axis=0)
        total = jnp.dot(left_ref[...], right, preferred_element_type=jnp.float32)
        refs[-1][...] = total.astype(jnp.bfloat16)

    flops = 2 * left.shape[0] * left.shape[1] * width
    return pl.pallas_call(
        kernel,
        grid=(width // tile,),
        in_specs=[whole(left.shape)]
        + [pl.BlockSpec((rows, tile), lambda j: (0, j)) for _ in blocks],
        out_specs=pl.BlockSpec((left.shape[0], tile), lambda j: (0, j)),
        out_shape=jax.ShapeDtypeStruct((left.shape[0], width), jnp.bfloat16),
        cost_estimate=pl.CostEstimate(
            flops=flops,
            bytes_accessed=2 * (left.size + 2 * blocks[0].size * len(blocks)),
            transcendentals=0,
        ),
        name="summed_product",
    )(left, *blocks)


def hidden_products(weights, place, first, second):
    rows, width = first[0].shape
    count = len(first)
    hidden = weights[0].shape[0]

    def kernel(place_ref, own_ref, other_ref, *refs):
        total_ref, rounded_ref = refs[2 * count :]
        spots = (place_ref[0], 1 - place_ref[0])
        for i in range(count):
            block = jnp.concatenate([refs[i][...], refs[count + i][...]], axis=1)
            for ref, spot in zip((own_ref, other_ref), spots):
                total = contract(ref[...], block, 1, 1)
                here = pl.ds(pl.multiple_of(spot * hidden, hidden), hidden)
                total_ref[here, i * rows : (i + 1) * rows] = total
                rounded_ref[here, i * rows : (i + 1) * rows] = total.astype(jnp.bfloat16)

    out = (2 * hidden, count * rows)
    return pl.pallas_call(
        kernel,
        grid_spec=pltpu.PrefetchScalarGridSpec(
            num_scalar_prefetch=1,
            grid=(1,),
            in_specs=[whole(weights[0].shape)] * 2 + [whole(first[0].shape)] * (2 * count),
            out_specs=[whole(out), whole(out)],
        ),
        out_shape=[jax.ShapeDtypeStruct(out, jnp.float32), jax.ShapeDtypeStruct(out, jnp.bfloat16)],
        cost_estimate=pl.CostEstimate(
            flops=8 * count * rows * width * hidden,
            bytes_accessed=4 * count * rows * width,
            transcendentals=0,
        ),
        name="hidden_products",
    )(place, *weights, *first, *second)


def forward(
    seen, held_pos, bases, window_starts, image_starts, w_turned, b_column, gain, bias, core, rows, piece
):
    count = bases.shape[0]
    _, window, feats = seen.shape
    window = 2 * window
    hidden = w_turned.shape[0]
    images = image_starts.shape[0]

    def own_half(array, core):
        lane = lax.broadcasted_iota(jnp.int32, (rows, 2 * piece), 1)
        first = core == 0
        kept = (lane < piece) == first
        held = []
        for i in range(0, feats, 4 * piece):
            left, right = array[:, i : i + 2 * piece], array[:, i + 2 * piece : i + 4 * piece]
            turned = pltpu.roll(jnp.where(first, right, left), piece, 1)
            held.append(jnp.where(kept, jnp.where(first, left, right), turned))
        return jnp.concatenate(held, axis=1)

    def kernel(base_ref, window_ref, image_ref, core_ref, seen_ref, pos_ref, w_ref, b_ref, gain_ref, bias_ref, own_gain_ref, own_bias_ref,
               in_ref, normed_ref, hidden_ref, slope_ref):
        step = pl.program_id(0)
        base = base_ref[step]
        begin = window_ref[step]
        own = base + lax.broadcasted_iota(jnp.int32, (rows, window), 0)
        select = (own == pos_ref[begin]).astype(jnp.float32).astype(jnp.bfloat16)
        held = seen_ref[pl.ds(begin, 2)].reshape(window, feats)
        placed = jnp.dot(select, held, preferred_element_type=jnp.float32)
        mean = jnp.mean(placed, axis=1, keepdims=True)
        centred = placed - mean
        var = jnp.mean(centred * centred, axis=1, keepdims=True)
        normed = centred * lax.rsqrt(var + 1e-05)
        normed_in = (normed * gain_ref[...] + bias_ref[...]).astype(jnp.bfloat16)
        own_normed = own_half(normed, core_ref[0])
        in_ref[...] = (own_normed * own_gain_ref[...] + own_bias_ref[...]).astype(jnp.bfloat16)
        normed_ref[...] = own_normed.astype(jnp.bfloat16)
        preact = contract(w_ref[...], normed_in, 1, 1) + b_ref[...]
        activ, slope = gelu_parts(preact)
        column = base + lax.broadcasted_iota(jnp.int32, (1, rows), 1)
        mask = jnp.zeros((1, rows), jnp.float32)
        for i in range(images):
            start = image_ref[i]
            inside = (column >= start) & (column < start + PATCH)
            mask = jnp.where(inside, 1.0, mask)
        hidden_ref[...] = (activ * mask).astype(jnp.bfloat16)
        slope_ref[...] = slope * mask

    positions = count * rows
    return pl.pallas_call(
        kernel,
        grid_spec=pltpu.PrefetchScalarGridSpec(
            num_scalar_prefetch=4,
            grid=(count,),
            in_specs=[
                whole(seen.shape),
                whole(held_pos.shape),
                whole(w_turned.shape),
                whole((hidden, 1)),
                whole((1, feats)),
                whole((1, feats)),
                whole((1, feats // 2)),
                whole((1, feats // 2)),
            ],
            out_specs=[
                pl.BlockSpec((rows, feats // 2), lambda i, *_: (i, 0)),
                pl.BlockSpec((rows, feats // 2), lambda i, *_: (i, 0)),
                pl.BlockSpec((hidden, rows), lambda i, *_: (0, i)),
                pl.BlockSpec((hidden, rows), lambda i, *_: (0, i)),
            ],
        ),
        out_shape=[
            jax.ShapeDtypeStruct((positions, feats // 2), jnp.bfloat16),
            jax.ShapeDtypeStruct((positions, feats // 2), jnp.bfloat16),
            jax.ShapeDtypeStruct((hidden, positions), jnp.bfloat16),
            jax.ShapeDtypeStruct((hidden, positions), jnp.float32),
        ],
        cost_estimate=pl.CostEstimate(
            flops=2 * positions * feats * (window + hidden),
            bytes_accessed=20 * positions * hidden,
            transcendentals=2 * positions * hidden,
        ),
        name="forward",
    )(bases, window_starts, image_starts, core, seen, held_pos, w_turned, b_column, gain[0], bias[0], gain[1], bias[1])


TILE = 256


def preact_grads(parts, others, slope_ref, held_ref, groups, rows):
    at = 0
    for part, other, group in zip(parts, others, groups):
        for i, block in enumerate(group):
            here = slice(i * rows, (i + 1) * rows)
            total = part[:, here] + other[:, here].astype(jnp.float32)
            total = total * slope_ref[:, block * rows : (block + 1) * rows]
            held_ref[:, at * rows : (at + 1) * rows] = total.astype(jnp.bfloat16)
            at += 1


def of_groups(ref, groups, rows):
    return jnp.concatenate(
        [ref[i * rows : (i + 1) * rows, :] for group in groups for i in group], axis=0
    )


def input_products(parts, others, slope, normed_in, normed, groups, rows):
    count = len(groups)
    hidden = slope.shape[0]
    held = rows * sum(len(group) for group in groups)
    positions, feats = normed_in.shape

    def kernel(*refs):
        parts, others = refs[:count], refs[count : 2 * count]
        slope_ref, in_ref, normed_ref, w_out, g_out, b_out, held_ref = refs[2 * count :]

        @pl.when(pl.program_id(0) == 0)
        def _():
            preact_grads(parts, others, slope_ref, held_ref, groups, rows)
            ones = jnp.ones((8, held), jnp.bfloat16)
            b_out[...] = contract(ones, held_ref[...], 1, 1)

        grads = held_ref[...]
        w_out[...] = jnp.dot(
            grads, of_groups(in_ref, groups, rows), preferred_element_type=jnp.float32
        )
        g_out[...] = jnp.dot(
            grads, of_groups(normed_ref, groups, rows), preferred_element_type=jnp.float32
        )

    column = pl.BlockSpec((positions, TILE), lambda j: (0, j))
    tile = pl.BlockSpec((hidden, TILE), lambda j: (0, j))
    return pl.pallas_call(
        kernel,
        grid=(feats // TILE,),
        in_specs=[whole(a.shape) for a in (*parts, *others)] + [whole(slope.shape), column, column],
        out_specs=[tile, tile, whole((8, hidden))],
        out_shape=[
            jax.ShapeDtypeStruct((hidden, feats), jnp.float32),
            jax.ShapeDtypeStruct((hidden, feats), jnp.float32),
            jax.ShapeDtypeStruct((8, hidden), jnp.float32),
        ],
        scratch_shapes=[pltpu.VMEM((hidden, held), jnp.bfloat16)],
        cost_estimate=pl.CostEstimate(
            flops=4 * held * hidden * feats, bytes_accessed=8 * positions * feats, transcendentals=0
        ),
        name="input_products",
    )(*parts, *others, slope, normed_in, normed)


def input_pieces(part, other, slope, normed_in, normed, before, w_own, out_rows, rows, at, images):
    hidden, held = part.shape
    own_feats = normed_in.shape[1]
    piece = own_feats // images
    width = hidden // 2
    steps = own_feats // TILE
    per_step = images // steps
    b_rows = hidden // TILE
    total_rows = 2 * steps + b_rows + out_rows.shape[0]
    padded = -(-total_rows // 8) * 8

    def kernel(part_ref, other_ref, slope_ref, in_ref, normed_ref, w_before, g_before, b_before,
               w_ref, rows_ref, sent_ref, held_ref, vector_ref, column_ref):
        step = pl.program_id(0)

        @pl.when(step == 0)
        def _():
            preact_grads([part_ref], [other_ref], slope_ref, held_ref, [range(held // rows)], rows)
            ones = jnp.ones((8, held), jnp.bfloat16)
            sums = contract(ones, held_ref[...], 1, 1) + b_before[...]
            vector_ref[...] = jnp.zeros_like(vector_ref)
            for i in range(b_rows):
                vector_ref[2 * steps + i : 2 * steps + i + 1, :] = sums[
                    0:1, i * TILE : (i + 1) * TILE
                ]
            first = 2 * steps + b_rows
            vector_ref[first : first + rows_ref.shape[0], :] = rows_ref[...]
            column_ref[...] = jnp.broadcast_to(sums[0:1, :], (128, hidden)).T

        grads = held_ref[...]
        w_grad = w_before[...] + jnp.dot(grads, in_ref[...], preferred_element_type=jnp.float32)
        g_grad = g_before[...] + jnp.dot(grads, normed_ref[...], preferred_element_type=jnp.float32)
        turned = w_grad.T.astype(jnp.bfloat16)
        for i in range(per_step):
            for half in range(2):
                sent_ref[half * images + step * per_step + i, 0:piece, :] = turned[
                    i * piece : (i + 1) * piece, half * width : (half + 1) * width
                ]
        weights = w_ref[...].astype(jnp.float32)
        column = jnp.concatenate([column_ref[...]] * (TILE // 128), axis=1)
        vector_ref[pl.ds(step, 1), :] = jnp.sum(g_grad * weights, axis=0, keepdims=True)
        vector_ref[pl.ds(steps + step, 1), :] = jnp.sum(column * weights, axis=0, keepdims=True)

        @pl.when(step == steps - 1)
        def _():
            vectors = vector_ref[...]
            high = vectors.astype(jnp.bfloat16).astype(jnp.float32)
            both = jnp.concatenate([high, vectors - high], axis=0).astype(jnp.bfloat16)
            for i in range(2 * images):
                sent_ref[i, piece : piece + 2 * padded, :] = both

    column = pl.BlockSpec((held, TILE), lambda j: (at, j))
    tile = pl.BlockSpec((hidden, TILE), lambda j: (0, j))
    sent = (2 * images, piece + 2 * padded, width)
    return pl.pallas_call(
        kernel,
        grid=(steps,),
        in_specs=[
            whole(part.shape),
            whole(part.shape),
            pl.BlockSpec((hidden, held), lambda j: (0, at)),
            column,
            column,
            tile,
            tile,
            whole((8, hidden)),
            tile,
            whole(out_rows.shape),
        ],
        out_specs=whole(sent),
        scratch_shapes=[
            pltpu.VMEM((hidden, held), jnp.bfloat16),
            pltpu.VMEM((padded, TILE), jnp.float32),
            pltpu.VMEM((hidden, 128), jnp.float32),
        ],
        out_shape=jax.ShapeDtypeStruct(sent, jnp.bfloat16),
        cost_estimate=pl.CostEstimate(
            flops=4 * held * hidden * own_feats, bytes_accessed=8 * held * own_feats, transcendentals=0
        ),
        name="input_pieces",
    )(part, other, slope, normed_in, normed, *before, w_own, out_rows)


def split_terms(vector):
    high = vector.astype(jnp.bfloat16)
    low = (vector - high.astype(jnp.float32)).astype(jnp.bfloat16)
    return high, low


def one_step(vision_feats, ln_gain, ln_bias, w_in, b_in, w_out, lm_grad, image_counts, token_pos):
    z_count = lax.axis_size("z")
    z = lax.axis_index("z")
    xl = lax.axis_index("xl")
    core = lax.axis_index("c")
    vision = vision_feats[0]
    lm = lm_grad[0]
    rows, half_width = lm.shape
    feats = vision.shape[1]
    quarter = half_width // 2
    counts = image_counts[0]
    positions = token_pos[0]
    tokens = positions.shape[0]
    image_index = jnp.arange(tokens, dtype=jnp.int32) // PATCH
    abs_pos = jnp.where(image_index >= counts[0], LEN, 0) + positions
    copies = jnp.broadcast_to(vision, (z_count, *vision.shape))
    seen = lax.all_to_all(copies, "z", 0, 0, tiled=True)
    low, high = [None] * z_count, [None] * z_count
    low[0], high[0] = lm[:, :quarter], lm[:, quarter:]
    low[7], low[1] = along_z(low[0], 1), along_z(low[0], -1)
    high[7], high[1] = along_z(high[0], 1), along_z(high[0], -1)
    w_out_other = swap(w_out, "xl")
    terms = split_terms(b_in)
    third = (b_in - terms[0].astype(jnp.float32) - terms[1].astype(jnp.float32)).astype(jnp.bfloat16)
    w_in_other = swap(w_in, "c")
    w_first, w_second = in_axis_order(w_in, w_in_other, "c")
    packed = jnp.concatenate(
        [w_first, w_second, jnp.stack([*terms, third]), jnp.zeros((5, b_in.shape[0]), jnp.bfloat16)]
    )
    packed_other = swap(packed, "xl")
    hidden_width = 2 * w_out.shape[0]
    plane_count = lax.axis_size(PLANE)
    img_count = lax.axis_size(IMG)
    piece = feats // (img_count * 2)
    packed = jnp.concatenate(in_axis_order(packed, packed_other, "xl"), axis=1)
    w_turned = packed[:feats].T
    w_own = packed[:feats].reshape(img_count, 2, piece, hidden_width)
    w_own = lax.dynamic_index_in_dim(w_own, core, 1, False).reshape(feats // 2, hidden_width).T
    b_column = jnp.sum(packed[feats : feats + 3].astype(jnp.float32), axis=0)[:, None]
    block_of = lax.rem(z + jnp.arange(z_count, dtype=jnp.int32), z_count)
    bases = (2 * block_of + xl) * rows
    image_starts = abs_pos[::PATCH]
    first_token = jnp.sum((abs_pos[None, :] < bases[:, None]).astype(jnp.int32), axis=1)
    of_z = tokens // z_count
    window_starts = jnp.minimum(first_token // of_z, z_count - 2)
    held_pos = abs_pos.reshape(z_count, 2, 2, of_z // 4)
    held_pos = jnp.where(xl == 0, held_pos, held_pos[:, ::-1])
    held_pos = jnp.where(core == 0, held_pos, held_pos[:, :, ::-1])
    held_pos = held_pos.transpose(0, 2, 1, 3).reshape(z_count, 1, of_z)
    own_pos = bases[0] + jnp.arange(rows, dtype=jnp.int32)
    inside = (own_pos[:, None] >= image_starts) & (own_pos[:, None] < image_starts + PATCH)
    mask = jnp.any(inside, axis=1).astype(jnp.bfloat16)
    out_part = jnp.dot(mask[None, :], lm, preferred_element_type=jnp.float32).reshape(-1, TILE)
    held_pos = jnp.concatenate([held_pos[:-1], held_pos[1:]], axis=2)

    def own_part(vector):
        parts = vector.reshape(img_count, 2, piece)
        return lax.dynamic_index_in_dim(parts, core, 1, False).reshape(1, -1)

    seen_other = swap(seen, "xl")
    gains = (ln_gain[None, :], own_part(ln_gain))
    biases = (ln_bias[None, :], own_part(ln_bias))
    low[7], low[1], w_turned, w_own, b_column, out_part, held_pos, window_starts, gains, biases = gate(
        low[7], low[1], w_turned, w_own, b_column, out_part, held_pos, window_starts, gains, biases
    )
    low[6], low[2] = along_z(low[7], 1), along_z(low[1], -1)
    high[7], high[1] = gate(high[7], high[1])
    high[6], high[2] = along_z(high[7], 1), along_z(high[1], -1)
    weights, place = (w_out, w_out_other), xl.reshape(1)

    def products(blocks):
        return hidden_products(weights, place, [low[i] for i in blocks], [high[i] for i in blocks])

    groups = [(7, 1), (6, 2), (5, 3), (0,)]
    parts, others = [None] * 4, [None] * 4
    parts[3], rounded_own = products(groups[3])
    parts[3], rounded_own, seen_other = gate(parts[3], rounded_own, seen_other)
    seen = jnp.stack([seen, seen_other], axis=1)
    seen_other = swap(seen, "c")
    others[3] = swap(rounded_own, "c")
    low[6], low[2] = gate(low[6], low[2])
    low[5], low[3] = along_z(low[6], 1), along_z(low[2], -1)
    parts[0], rounded = products(groups[0])
    others[0] = swap(rounded, "c")
    seen = jnp.stack([seen, seen_other], axis=1).reshape(z_count, of_z, feats)
    normed_in, normed, hidden, slope = forward(
        seen,
        held_pos,
        bases,
        window_starts,
        image_starts,
        w_turned,
        b_column,
        gains,
        biases,
        core.reshape(1),
        rows,
        piece,
    )
    high[6], high[2] = gate(high[6], high[2])
    high[5], high[3] = along_z(high[6], 1), along_z(high[2], -1)
    low[5], low[3], hidden, others[0], others[3] = gate(
        low[5], low[3], hidden, others[0], others[3]
    )
    low[4] = along_z(low[5], 1)
    parts[1], rounded = products(groups[1])
    others[1] = swap(rounded, "c")
    high[5], high[3], parts[1] = gate(high[5], high[3], parts[1])
    high[4] = along_z(high[3], -1)
    parts[2], rounded = products(groups[2])
    others[2] = swap(rounded, "c")
    low[4], hidden, parts[2], rounded = gate(low[4], hidden, parts[2], rounded)
    low_product = summed_product(hidden, low)
    low_product, normed_in, normed, slope = gate(low_product, normed_in, normed, slope)
    low_moved = lax.all_to_all(low_product, PLANE, 0, 0, tiled=True)
    before = input_products(parts, others, slope, normed_in, normed, groups, rows)
    high[4], *before = gate(high[4], *before)
    part, rounded = products((4,))
    other = swap(rounded, "c")
    high_product = summed_product(hidden, high)
    sent = input_pieces(
        part, other, slope, normed_in, normed, before, w_own, out_part, rows, 4, img_count
    )
    sent, low_moved = gate(sent, low_moved)
    moved = lax.all_to_all(sent, PLANE, 0, 0, tiled=True)
    moved, high_product = gate(moved, high_product)
    high_moved = lax.all_to_all(high_product, PLANE, 0, 0, tiled=True)
    summed = jnp.sum(moved.astype(jnp.float32), axis=0)
    w_in_grad = summed[:piece]
    padded = (summed.shape[0] - piece) // 2
    vectors = summed[piece : piece + padded] + summed[piece + padded :]
    line = feats // 2 // TILE
    b_lines = hidden_width // TILE
    out_lines = half_width // TILE
    b_own = vectors[2 * line : 2 * line + b_lines]
    b_full = jnp.where((jnp.arange(z_count) == z)[:, None, None], b_own[None], 0.0)
    vectors = jnp.concatenate(
        [
            vectors[: 2 * line],
            vectors[2 * line + b_lines : 2 * line + b_lines + out_lines],
            b_full.reshape(-1, TILE),
        ]
    )
    for shift in (1, 2, 4):
        moved = lax.ppermute(vectors, "z", [(i, i ^ shift) for i in range(z_count)])
        vectors = vectors + moved
    first, second = in_axis_order(vectors, swap(vectors, "c"), "c")

    def by_core(low_half, high_half):
        return jnp.stack([low_half.reshape(-1, piece), high_half.reshape(-1, piece)], 1).reshape(-1)

    gain_grad = by_core(first[:line], second[:line])
    bias_grad = by_core(first[line : 2 * line], second[line : 2 * line])
    out_end = 2 * line + out_lines
    b_out_grad = jnp.concatenate([first[2 * line : out_end], second[2 * line : out_end]]).reshape(-1)
    b_in_grad = first[out_end:].reshape(-1)

    def over_plane(array):
        return jnp.sum(array.reshape(plane_count, -1, quarter).astype(jnp.float32), axis=0)

    w_out_grad = jnp.concatenate([over_plane(low_moved), over_plane(high_moved)], axis=1)
    return (w_in_grad, b_in_grad, w_out_grad, b_out_grad, gain_grad, bias_grad)


def solution(mesh):
    finer = Mesh(
        mesh.devices.reshape(8, 2, 4, 2, mesh.shape["fsdp"]),
        ("z", "xl", "y", "xh", "c"),
    )
    placed = (
        P(IMG, ("z", "xl", "c"), None),
        P(),
        P(),
        P("c", SEQ),
        P(SEQ),
        P(SEQ, "c"),
        P(IMG, SEQ, "c"),
        P(IMG, None),
        P(IMG, None),
    )

    return jax.shard_map(
        one_step,
        mesh=finer,
        in_specs=placed,
        out_specs=(P(("y", "xh", "c"), SEQ), P(), P(("z", "xl", "y", "xh"), "c"), P(), P(), P()),
        check_vma=False,
    )
```

```python
import jax
import jax.numpy as jnp
from jax import lax
from jax.experimental import pallas as pl
from jax.experimental.pallas import tpu as pltpu
from jax.sharding import Mesh
from jax.sharding import PartitionSpec as P

PATCH = 576
LEN = 2048
SEQ = ("z", "xl")
IMG = ("y", "xh")
PLANE = ("xl", "y", "xh")


def gelu_parts(preact):
    cumul = 0.5 * (1.0 + lax.erf(preact * 0.7071067811865476))
    density = jnp.exp(-0.5 * preact * preact) * 0.3989422804014327
    return (preact * cumul, cumul + preact * density)


def contract(left, right, left_dim, right_dim):
    return lax.dot_general(
        left, right, (((left_dim,), (right_dim,)), ((), ())), preferred_element_type=jnp.float32
    )


def swap(array, axis):
    return lax.ppermute(array, axis, [(0, 1), (1, 0)])


def in_axis_order(own, other, axis):
    first = lax.axis_index(axis) == 0
    return jnp.where(first, own, other), jnp.where(first, other, own)


def along_z(array, shift):
    count = lax.axis_size("z")
    return lax.ppermute(array, "z", [(i, (i + shift) % count) for i in range(count)])


def gate(*values):
    return lax.optimization_barrier(values)


def whole(shape):
    return pl.BlockSpec(shape, lambda *_: (0,) * len(shape))


def summed_product(left, blocks):
    rows, width = blocks[0].shape
    tile = width // 2

    def kernel(left_ref, *refs):
        right = jnp.concatenate([ref[...] for ref in refs[:-1]], axis=0)
        total = jnp.dot(left_ref[...], right, preferred_element_type=jnp.float32)
        refs[-1][...] = total.astype(jnp.bfloat16)

    flops = 2 * left.shape[0] * left.shape[1] * width
    return pl.pallas_call(
        kernel,
        grid=(width // tile,),
        in_specs=[whole(left.shape)]
        + [pl.BlockSpec((rows, tile), lambda j: (0, j)) for _ in blocks],
        out_specs=pl.BlockSpec((left.shape[0], tile), lambda j: (0, j)),
        out_shape=jax.ShapeDtypeStruct((left.shape[0], width), jnp.bfloat16),
        cost_estimate=pl.CostEstimate(
            flops=flops,
            bytes_accessed=2 * (left.size + 2 * blocks[0].size * len(blocks)),
            transcendentals=0,
        ),
        name="summed_product",
    )(left, *blocks)


def hidden_products(weights, place, first, second):
    rows, width = first[0].shape
    count = len(first)
    hidden = weights[0].shape[0]

    def kernel(place_ref, own_ref, other_ref, *refs):
        total_ref, rounded_ref = refs[2 * count :]
        spots = (place_ref[0], 1 - place_ref[0])
        for i in range(count):
            block = jnp.concatenate([refs[i][...], refs[count + i][...]], axis=1)
            for ref, spot in zip((own_ref, other_ref), spots):
                total = contract(ref[...], block, 1, 1)
                here = pl.ds(pl.multiple_of(spot * hidden, hidden), hidden)
                total_ref[here, i * rows : (i + 1) * rows] = total
                rounded_ref[here, i * rows : (i + 1) * rows] = total.astype(jnp.bfloat16)

    out = (2 * hidden, count * rows)
    return pl.pallas_call(
        kernel,
        grid_spec=pltpu.PrefetchScalarGridSpec(
            num_scalar_prefetch=1,
            grid=(1,),
            in_specs=[whole(weights[0].shape)] * 2 + [whole(first[0].shape)] * (2 * count),
            out_specs=[whole(out), whole(out)],
        ),
        out_shape=[jax.ShapeDtypeStruct(out, jnp.float32), jax.ShapeDtypeStruct(out, jnp.bfloat16)],
        cost_estimate=pl.CostEstimate(
            flops=8 * count * rows * width * hidden,
            bytes_accessed=4 * count * rows * width,
            transcendentals=0,
        ),
        name="hidden_products",
    )(place, *weights, *first, *second)


def forward(
    seen, held_pos, bases, window_starts, image_starts, w_turned, b_column, gain, bias, core, rows, piece
):
    count = bases.shape[0]
    _, window, feats = seen.shape
    window = 2 * window
    hidden = w_turned.shape[0]
    images = image_starts.shape[0]

    def own_half(array, core):
        lane = lax.broadcasted_iota(jnp.int32, (rows, 2 * piece), 1)
        first = core == 0
        kept = (lane < piece) == first
        held = []
        for i in range(0, feats, 4 * piece):
            left, right = array[:, i : i + 2 * piece], array[:, i + 2 * piece : i + 4 * piece]
            turned = pltpu.roll(jnp.where(first, right, left), piece, 1)
            held.append(jnp.where(kept, jnp.where(first, left, right), turned))
        return jnp.concatenate(held, axis=1)

    def kernel(base_ref, window_ref, image_ref, core_ref, seen_ref, pos_ref, w_ref, b_ref, gain_ref, bias_ref, own_gain_ref, own_bias_ref,
               in_ref, normed_ref, hidden_ref, slope_ref):
        step = pl.program_id(0)
        base = base_ref[step]
        begin = window_ref[step]
        own = base + lax.broadcasted_iota(jnp.int32, (rows, window), 0)
        select = (own == pos_ref[begin]).astype(jnp.float32).astype(jnp.bfloat16)
        held = seen_ref[pl.ds(begin, 2)].reshape(window, feats)
        placed = jnp.dot(select, held, preferred_element_type=jnp.float32)
        mean = jnp.mean(placed, axis=1, keepdims=True)
        centred = placed - mean
        var = jnp.mean(centred * centred, axis=1, keepdims=True)
        normed = centred * lax.rsqrt(var + 1e-05)
        normed_in = (normed * gain_ref[...] + bias_ref[...]).astype(jnp.bfloat16)
        own_normed = own_half(normed, core_ref[0])
        in_ref[...] = (own_normed * own_gain_ref[...] + own_bias_ref[...]).astype(jnp.bfloat16)
        normed_ref[...] = own_normed.astype(jnp.bfloat16)
        preact = contract(w_ref[...], normed_in, 1, 1) + b_ref[...]
        activ, slope = gelu_parts(preact)
        column = base + lax.broadcasted_iota(jnp.int32, (1, rows), 1)
        mask = jnp.zeros((1, rows), jnp.float32)
        for i in range(images):
            start = image_ref[i]
            inside = (column >= start) & (column < start + PATCH)
            mask = jnp.where(inside, 1.0, mask)
        hidden_ref[...] = (activ * mask).astype(jnp.bfloat16)
        slope_ref[...] = slope * mask

    positions = count * rows
    return pl.pallas_call(
        kernel,
        grid_spec=pltpu.PrefetchScalarGridSpec(
            num_scalar_prefetch=4,
            grid=(count,),
            in_specs=[
                whole(seen.shape),
                whole(held_pos.shape),
                whole(w_turned.shape),
                whole((hidden, 1)),
                whole((1, feats)),
                whole((1, feats)),
                whole((1, feats // 2)),
                whole((1, feats // 2)),
            ],
            out_specs=[
                pl.BlockSpec((rows, feats // 2), lambda i, *_: (i, 0)),
                pl.BlockSpec((rows, feats // 2), lambda i, *_: (i, 0)),
                pl.BlockSpec((hidden, rows), lambda i, *_: (0, i)),
                pl.BlockSpec((hidden, rows), lambda i, *_: (0, i)),
            ],
        ),
        out_shape=[
            jax.ShapeDtypeStruct((positions, feats // 2), jnp.bfloat16),
            jax.ShapeDtypeStruct((positions, feats // 2), jnp.bfloat16),
            jax.ShapeDtypeStruct((hidden, positions), jnp.bfloat16),
            jax.ShapeDtypeStruct((hidden, positions), jnp.float32),
        ],
        cost_estimate=pl.CostEstimate(
            flops=2 * positions * feats * (window + hidden),
            bytes_accessed=20 * positions * hidden,
            transcendentals=2 * positions * hidden,
        ),
        name="forward",
    )(bases, window_starts, image_starts, core, seen, held_pos, w_turned, b_column, gain[0], bias[0], gain[1], bias[1])


TILE = 256


def preact_grads(parts, others, slope_ref, held_ref, groups, rows):
    at = 0
    for part, other, group in zip(parts, others, groups):
        for i, block in enumerate(group):
            here = slice(i * rows, (i + 1) * rows)
            total = part[:, here] + other[:, here].astype(jnp.float32)
            total = total * slope_ref[:, block * rows : (block + 1) * rows]
            held_ref[:, at * rows : (at + 1) * rows] = total.astype(jnp.bfloat16)
            at += 1


def of_groups(ref, groups, rows):
    return jnp.concatenate(
        [ref[i * rows : (i + 1) * rows, :] for group in groups for i in group], axis=0
    )


def input_pieces(parts, others, slope, normed_in, normed, w_own, out_rows, groups, rows, images):
    count = len(groups)
    hidden, held = slope.shape
    own_feats = normed_in.shape[1]
    piece = own_feats // images
    width = hidden // 2
    steps = own_feats // TILE
    per_step = images // steps
    b_rows = hidden // TILE
    total_rows = 2 * steps + b_rows + out_rows.shape[0]
    padded = -(-total_rows // 8) * 8

    def kernel(*refs):
        parts, others = refs[:count], refs[count : 2 * count]
        slope_ref, in_ref, normed_ref, w_ref, rows_ref = refs[2 * count : 2 * count + 5]
        sent_ref, held_ref, vector_ref, column_ref = refs[2 * count + 5 :]
        step = pl.program_id(0)

        @pl.when(step == 0)
        def _():
            preact_grads(parts, others, slope_ref, held_ref, groups, rows)
            ones = jnp.ones((8, held), jnp.bfloat16)
            sums = contract(ones, held_ref[...], 1, 1)
            vector_ref[...] = jnp.zeros_like(vector_ref)
            for i in range(b_rows):
                vector_ref[2 * steps + i : 2 * steps + i + 1, :] = sums[
                    0:1, i * TILE : (i + 1) * TILE
                ]
            first = 2 * steps + b_rows
            vector_ref[first : first + rows_ref.shape[0], :] = rows_ref[...]
            column_ref[...] = jnp.broadcast_to(sums[0:1, :], (128, hidden)).T

        grads = held_ref[...]
        w_grad = jnp.dot(
            grads, of_groups(in_ref, groups, rows), preferred_element_type=jnp.float32
        )
        g_grad = jnp.dot(
            grads, of_groups(normed_ref, groups, rows), preferred_element_type=jnp.float32
        )
        turned = w_grad.T.astype(jnp.bfloat16)
        for i in range(per_step):
            for half in range(2):
                sent_ref[half * images + step * per_step + i, 0:piece, :] = turned[
                    i * piece : (i + 1) * piece, half * width : (half + 1) * width
                ]
        weights = w_ref[...].astype(jnp.float32)
        column = jnp.concatenate([column_ref[...]] * (TILE // 128), axis=1)
        vector_ref[pl.ds(step, 1), :] = jnp.sum(g_grad * weights, axis=0, keepdims=True)
        vector_ref[pl.ds(steps + step, 1), :] = jnp.sum(column * weights, axis=0, keepdims=True)

        @pl.when(step == steps - 1)
        def _():
            vectors = vector_ref[...]
            high = vectors.astype(jnp.bfloat16).astype(jnp.float32)
            both = jnp.concatenate([high, vectors - high], axis=0).astype(jnp.bfloat16)
            for i in range(2 * images):
                sent_ref[i, piece : piece + 2 * padded, :] = both

    column = pl.BlockSpec((held, TILE), lambda j: (0, j))
    tile = pl.BlockSpec((hidden, TILE), lambda j: (0, j))
    sent = (2 * images, piece + 2 * padded, width)
    return pl.pallas_call(
        kernel,
        grid=(steps,),
        in_specs=[whole(a.shape) for a in (*parts, *others)]
        + [whole(slope.shape), column, column, tile, whole(out_rows.shape)],
        out_specs=whole(sent),
        scratch_shapes=[
            pltpu.VMEM((hidden, held), jnp.bfloat16),
            pltpu.VMEM((padded, TILE), jnp.float32),
            pltpu.VMEM((hidden, 128), jnp.float32),
        ],
        out_shape=jax.ShapeDtypeStruct(sent, jnp.bfloat16),
        cost_estimate=pl.CostEstimate(
            flops=4 * held * hidden * own_feats, bytes_accessed=8 * held * own_feats, transcendentals=0
        ),
        name="input_pieces",
    )(*parts, *others, slope, normed_in, normed, w_own, out_rows)


def split_terms(vector):
    high = vector.astype(jnp.bfloat16)
    low = (vector - high.astype(jnp.float32)).astype(jnp.bfloat16)
    return high, low


def one_step(vision_feats, ln_gain, ln_bias, w_in, b_in, w_out, lm_grad, image_counts, token_pos):
    z_count = lax.axis_size("z")
    z = lax.axis_index("z")
    xl = lax.axis_index("xl")
    core = lax.axis_index("c")
    vision = vision_feats[0]
    lm = lm_grad[0]
    rows, half_width = lm.shape
    feats = vision.shape[1]
    quarter = half_width // 2
    counts = image_counts[0]
    positions = token_pos[0]
    tokens = positions.shape[0]
    image_index = jnp.arange(tokens, dtype=jnp.int32) // PATCH
    abs_pos = jnp.where(image_index >= counts[0], LEN, 0) + positions
    copies = jnp.broadcast_to(vision, (z_count, *vision.shape))
    seen = lax.all_to_all(copies, "z", 0, 0, tiled=True)
    low, high = [None] * z_count, [None] * z_count
    low[0], high[0] = lm[:, :quarter], lm[:, quarter:]
    low[7], low[1] = along_z(low[0], 1), along_z(low[0], -1)
    high[7], high[1] = along_z(high[0], 1), along_z(high[0], -1)
    w_out_other = swap(w_out, "xl")
    terms = split_terms(b_in)
    third = (b_in - terms[0].astype(jnp.float32) - terms[1].astype(jnp.float32)).astype(jnp.bfloat16)
    w_in_other = swap(w_in, "c")
    w_first, w_second = in_axis_order(w_in, w_in_other, "c")
    packed = jnp.concatenate(
        [w_first, w_second, jnp.stack([*terms, third]), jnp.zeros((5, b_in.shape[0]), jnp.bfloat16)]
    )
    packed_other = swap(packed, "xl")
    hidden_width = 2 * w_out.shape[0]
    plane_count = lax.axis_size(PLANE)
    img_count = lax.axis_size(IMG)
    piece = feats // (img_count * 2)
    packed = jnp.concatenate(in_axis_order(packed, packed_other, "xl"), axis=1)
    w_turned = packed[:feats].T
    w_own = packed[:feats].reshape(img_count, 2, piece, hidden_width)
    w_own = lax.dynamic_index_in_dim(w_own, core, 1, False).reshape(feats // 2, hidden_width).T
    b_column = jnp.sum(packed[feats : feats + 3].astype(jnp.float32), axis=0)[:, None]
    block_of = lax.rem(z + jnp.arange(z_count, dtype=jnp.int32), z_count)
    bases = (2 * block_of + xl) * rows
    image_starts = abs_pos[::PATCH]
    first_token = jnp.sum((abs_pos[None, :] < bases[:, None]).astype(jnp.int32), axis=1)
    of_z = tokens // z_count
    window_starts = jnp.minimum(first_token // of_z, z_count - 2)
    held_pos = abs_pos.reshape(z_count, 2, 2, of_z // 4)
    held_pos = jnp.where(xl == 0, held_pos, held_pos[:, ::-1])
    held_pos = jnp.where(core == 0, held_pos, held_pos[:, :, ::-1])
    held_pos = held_pos.transpose(0, 2, 1, 3).reshape(z_count, 1, of_z)
    own_pos = bases[0] + jnp.arange(rows, dtype=jnp.int32)
    inside = (own_pos[:, None] >= image_starts) & (own_pos[:, None] < image_starts + PATCH)
    mask = jnp.any(inside, axis=1).astype(jnp.bfloat16)
    out_part = jnp.dot(mask[None, :], lm, preferred_element_type=jnp.float32).reshape(-1, TILE)
    held_pos = jnp.concatenate([held_pos[:-1], held_pos[1:]], axis=2)

    def own_part(vector):
        parts = vector.reshape(img_count, 2, piece)
        return lax.dynamic_index_in_dim(parts, core, 1, False).reshape(1, -1)

    seen_other = swap(seen, "xl")
    gains = (ln_gain[None, :], own_part(ln_gain))
    biases = (ln_bias[None, :], own_part(ln_bias))
    low[7], low[1], w_turned, w_own, b_column, out_part, held_pos, window_starts, gains, biases = gate(
        low[7], low[1], w_turned, w_own, b_column, out_part, held_pos, window_starts, gains, biases
    )
    low[6], low[2] = along_z(low[7], 1), along_z(low[1], -1)
    high[7], high[1] = gate(high[7], high[1])
    high[6], high[2] = along_z(high[7], 1), along_z(high[1], -1)
    weights, place = (w_out, w_out_other), xl.reshape(1)

    def products(blocks):
        return hidden_products(weights, place, [low[i] for i in blocks], [high[i] for i in blocks])

    groups = [(7, 1), (6, 2, 5, 3), (4,), (0,)]
    parts, others = [None] * 4, [None] * 4
    parts[3], rounded_own = products(groups[3])
    parts[3], rounded_own, seen_other = gate(parts[3], rounded_own, seen_other)
    seen = jnp.stack([seen, seen_other], axis=1)
    seen_other = swap(seen, "c")
    others[3] = swap(rounded_own, "c")
    low[6], low[2] = gate(low[6], low[2])
    low[5], low[3] = along_z(low[6], 1), along_z(low[2], -1)
    parts[0], rounded = products(groups[0])
    others[0] = swap(rounded, "c")
    seen = jnp.stack([seen, seen_other], axis=1).reshape(z_count, of_z, feats)
    normed_in, normed, hidden, slope = forward(
        seen,
        held_pos,
        bases,
        window_starts,
        image_starts,
        w_turned,
        b_column,
        gains,
        biases,
        core.reshape(1),
        rows,
        piece,
    )
    high[6], high[2] = gate(high[6], high[2])
    high[5], high[3] = along_z(high[6], 1), along_z(high[2], -1)
    low[5], low[3], hidden, others[0], others[3] = gate(
        low[5], low[3], hidden, others[0], others[3]
    )
    low[4] = along_z(low[5], 1)
    high[5], high[3], hidden = gate(high[5], high[3], hidden)
    high[4] = along_z(high[3], -1)
    parts[1], rounded = products(groups[1])
    others[1] = swap(rounded, "c")
    low[4], hidden, parts[1] = gate(low[4], hidden, parts[1])
    low_product = summed_product(hidden, low)
    high[4], low_product = gate(high[4], low_product)
    parts[2], rounded = products(groups[2])
    others[2] = swap(rounded, "c")
    low_product, normed_in, normed, slope, rounded = gate(
        low_product, normed_in, normed, slope, rounded
    )
    low_moved = lax.all_to_all(low_product, PLANE, 0, 0, tiled=True)
    high_product = summed_product(hidden, high)
    sent = input_pieces(
        parts, others, slope, normed_in, normed, w_own, out_part, groups, rows, img_count
    )
    sent, low_moved = gate(sent, low_moved)
    moved = lax.all_to_all(sent, PLANE, 0, 0, tiled=True)
    moved, high_product = gate(moved, high_product)
    high_moved = lax.all_to_all(high_product, PLANE, 0, 0, tiled=True)
    summed = jnp.sum(moved.astype(jnp.float32), axis=0)
    w_in_grad = summed[:piece]
    padded = (summed.shape[0] - piece) // 2
    vectors = summed[piece : piece + padded] + summed[piece + padded :]
    line = feats // 2 // TILE
    b_lines = hidden_width // TILE
    out_lines = half_width // TILE
    b_own = vectors[2 * line : 2 * line + b_lines]
    b_full = jnp.where((jnp.arange(z_count) == z)[:, None, None], b_own[None], 0.0)
    vectors = jnp.concatenate(
        [
            vectors[: 2 * line],
            vectors[2 * line + b_lines : 2 * line + b_lines + out_lines],
            b_full.reshape(-1, TILE),
        ]
    )
    for shift in (1, 2, 4):
        moved = lax.ppermute(vectors, "z", [(i, i ^ shift) for i in range(z_count)])
        vectors = vectors + moved
    first, second = in_axis_order(vectors, swap(vectors, "c"), "c")

    def by_core(low_half, high_half):
        return jnp.stack([low_half.reshape(-1, piece), high_half.reshape(-1, piece)], 1).reshape(-1)

    gain_grad = by_core(first[:line], second[:line])
    bias_grad = by_core(first[line : 2 * line], second[line : 2 * line])
    out_end = 2 * line + out_lines
    b_out_grad = jnp.concatenate([first[2 * line : out_end], second[2 * line : out_end]]).reshape(-1)
    b_in_grad = first[out_end:].reshape(-1)

    def over_plane(array):
        return jnp.sum(array.reshape(plane_count, -1, quarter).astype(jnp.float32), axis=0)

    w_out_grad = jnp.concatenate([over_plane(low_moved), over_plane(high_moved)], axis=1)
    return (w_in_grad, b_in_grad, w_out_grad, b_out_grad, gain_grad, bias_grad)


def solution(mesh):
    finer = Mesh(
        mesh.devices.reshape(8, 2, 4, 2, mesh.shape["fsdp"]),
        ("z", "xl", "y", "xh", "c"),
    )
    placed = (
        P(IMG, ("z", "xl", "c"), None),
        P(),
        P(),
        P("c", SEQ),
        P(SEQ),
        P(SEQ, "c"),
        P(IMG, SEQ, "c"),
        P(IMG, None),
        P(IMG, None),
    )

    return jax.shard_map(
        one_step,
        mesh=finer,
        in_specs=placed,
        out_specs=(P(("y", "xh", "c"), SEQ), P(), P(("z", "xl", "y", "xh"), "c"), P(), P(), P()),
        check_vma=False,
    )
```
